768 devices in a mesh: dp: 384 (over x, y, z), mp: 2 (over core).
Axes of the slice: x: 4, y: 8, z: 12, core: 2. Of those that a mesh axis runs over, the one named last changes fastest.
Arguments:
- attn: bfloat16 [147456, 1536], P('dp', 'mp'), may hold values from -6 to 6
- w_out: bfloat16 [1536, 1536], P('mp'), may hold values from -0.15625 to 0.15625
- resid: bfloat16 [147456, 1536], P('dp', 'mp'), may hold values from -6 to 6
- target: bfloat16 [147456, 1536], P('dp', 'mp'), may hold values from -6 to 6
- gate: float32 [1152, 1536], P('dp', 'mp'), may hold values from -5 to 5
- bins: int32 [1152], P('dp'), may hold values from 0 to 127
Outputs:
- grad_w_out: float32 [1536, 1536], P('dp', 'mp')
- grad_gate: float32 [1152, 1536], P('dp', 'mp')
- bin_loss: float32 [128], replicated
The draws below stay inside these ranges and needn't reach their ends.
All inputs are finite; a program needn't handle non-finite values.
Results may differ from the reference program's by a relative error of at most 0.0008.
Values may be sent and summed in bfloat16 or wider, within the bound.
No kernel may reach another device: no remote copies, remote signals or barrier semaphores. Data moves between devices by JAX's collectives and lax.ppermute only.
A program may use at most 32 MiB of HBM per device.

```python
import math
import jax
import jax.numpy as jnp
from jax import lax

D = 1536
NBINS = 128
SAMP_DEV = 3
TOK_SAMP = 128
SAMPLES = 1152
TOKENS = 147456
N_DP = 384


def plant(entries, stream_key, low, top_value):
    place = [jax.random.randint(jax.random.fold_in(stream_key, axis), (), 0, length) for axis, length in enumerate(entries.shape)]
    widest = entries.shape.index(max(entries.shape))
    neighbour = place[:widest] + [(place[widest] + 1) % entries.shape[widest]] + place[widest + 1:]
    return entries.at[tuple(place)].set(low).at[tuple(neighbour)].set(top_value)


def block_scale(stream_key, dims, shards, low, largest):
    gain, own = 1.0, jax.random.fold_in(stream_key, 6)
    for axis_at, shards_of in shards:
        heights = jnp.exp(jax.random.uniform(jax.random.fold_in(own, axis_at), (shards_of,), jnp.float32, low / len(shards), largest / len(shards)))
        gain = gain * jnp.repeat(heights, dims[axis_at] // shards_of).reshape([-1 if axis == axis_at else 1 for axis in range(len(dims))])
    return gain


def centred(stream_key, dims, width, bound, pieces=(), held_as=jnp.bfloat16):
    values = width * jax.random.normal(stream_key, dims, jnp.float32)
    if pieces:
        values = values * block_scale(stream_key, dims, pieces, -0.22, 0.18)
    return jnp.clip(values, -bound, bound).astype(held_as)


def setup_inputs(seed: int = 0) -> dict:
    streams_of = jax.random.split(jax.random.key(seed), 7)
    return {
        "attn": centred(streams_of[0], (TOKENS, D), 1.0, 6.0, ((0, 384), (1, 2))),
        "w_out": centred(streams_of[1], (D, D), D ** -0.5, 0.15625, ((0, 2),)),
        "resid": centred(streams_of[2], (TOKENS, D), 1.0, 6.0, ((0, 384), (1, 2))),
        "target": centred(streams_of[3], (TOKENS, D), 1.0, 6.0, ((0, 384), (1, 2))),
        "gate": centred(streams_of[4], (SAMPLES, D), 1.0, 5.0, ((0, 384), (1, 2)), jnp.float32),
        "bins": plant(jax.random.randint(streams_of[5], (SAMPLES,), 0, NBINS), jax.random.fold_in(streams_of[5], 1), 0, NBINS - 1).astype(jnp.int32),
    }


LOSS_SCALE = 4096.0

def bin_weights():
    centre = (jnp.arange(NBINS).astype(jnp.float32) + 0.5) / NBINS
    logit = jnp.log(centre) - jnp.log(1.0 - centre)
    return jnp.exp(-0.5 * logit * logit) / (math.sqrt(2.0 * math.pi) * centre * (1.0 - centre))

def reference(attn, w_out, resid, target, gate, bins):
    bin_ids = jnp.arange(NBINS, dtype=jnp.int32)
    one_hot = (bins[:, None] == bin_ids[None, :]).astype(jnp.float32)
    counts = lax.optimization_barrier(jnp.sum(one_hot, axis=0))
    floored = jnp.maximum(counts, 1.0)
    weights = bin_weights()
    scale_bin = LOSS_SCALE * weights / floored
    coefficient = lax.optimization_barrier(jnp.sum(one_hot * scale_bin[None, :], axis=1)) * (2.0 / (TOK_SAMP * D))
    tok_rows = SAMP_DEV * TOK_SAMP
    attn_blocks = attn.reshape(N_DP, tok_rows, D)
    resid_blocks = resid.reshape(N_DP, tok_rows, D)
    target_blocks = target.reshape(N_DP, tok_rows, D)
    gate_blocks = gate.reshape(N_DP, SAMP_DEV, D)
    coef_blocks = coefficient.reshape(N_DP, SAMP_DEV)

    def step(total, inputs):
        attn_in, resid_in, target_in, gate_in, coef_in = inputs
        projected = jnp.dot(attn_in, w_out, preferred_element_type=jnp.float32).reshape(SAMP_DEV, TOK_SAMP, D)
        hidden = resid_in.reshape(SAMP_DEV, TOK_SAMP, D).astype(jnp.float32) + gate_in[:, None, :] * projected
        error_cube = hidden - target_in.reshape(SAMP_DEV, TOK_SAMP, D).astype(jnp.float32)
        sample_error = lax.optimization_barrier(jnp.sum(error_cube * error_cube, axis=(1, 2))) / (TOK_SAMP * D)
        d_hidden = coef_in[:, None, None] * error_cube
        grad_gate = lax.optimization_barrier(jnp.sum(d_hidden * projected, axis=1))
        d_proj = (d_hidden * gate_in[:, None, :]).astype(jnp.bfloat16).reshape(tok_rows, D)
        total = total + lax.dot_general(attn_in, d_proj, (((0,), (0,)), ((), ())), preferred_element_type=jnp.float32)
        return (total, (sample_error, grad_gate))
    start_total = jnp.zeros((D, D), jnp.float32)
    total, (errors, grads) = lax.scan(step, start_total, (attn_blocks, resid_blocks, target_blocks, gate_blocks, coef_blocks))
    sums = lax.optimization_barrier(jnp.sum(one_hot * errors.reshape(-1)[:, None], axis=0))
    bin_loss = weights * sums / floored
    return (total, grads.reshape(SAMPLES, D), bin_loss)
```

```python
import math

import jax
import jax.numpy as jnp
from jax import lax
from jax.sharding import Mesh
from jax.sharding import PartitionSpec as P

NBINS = 128
DP = ("dp_0", "dp_1", "dp_2")
LOSS_SCALE = 4096.0
ATTN_BOUND = 6.0
TOP = 14.0
EXTRA = 8


def bin_weights():
    centre = (jnp.arange(NBINS).astype(jnp.float32) + 0.5) / NBINS
    logit = jnp.log(centre) - jnp.log(1.0 - centre)
    return jnp.exp(-0.5 * logit * logit) / (math.sqrt(2.0 * math.pi) * centre * (1.0 - centre))


def partner(x):
    return lax.ppermute(x, "mp", [(0, 1), (1, 0)])


def summed_everywhere(x, axes):
    size = math.prod(lax.axis_size(a) for a in ([axes] if isinstance(axes, str) else axes))
    spread = jnp.broadcast_to(x[None], (size, *x.shape))
    return jnp.sum(lax.all_to_all(spread, axes, 0, 0, tiled=True), axis=0)


def exponent_of(bound):
    return jnp.floor(jnp.log2(jnp.maximum(bound, 1e-30))) + 2.0


def side_rows(losses, bound_exp, cols):
    loss_exp = exponent_of(jnp.max(losses))
    scaled = losses * jnp.exp2(TOP - loss_exp)
    high = scaled.astype(jnp.float16)
    low = ((scaled - high.astype(jnp.float32)) * 1024.0).astype(jnp.float16)
    exps = jnp.concatenate(
        [jnp.broadcast_to(bound_exp, (NBINS,)), jnp.broadcast_to(loss_exp, (NBINS,))]
    ).astype(jnp.float16)
    row = jnp.concatenate([high, low, exps])
    return jnp.pad(row[None, :], ((0, EXTRA - 1), (0, cols - 4 * NBINS)))


def packed(total, losses, bound, size):
    rows, cols = total.shape
    bound_exp = exponent_of(bound)
    body = (total * jnp.exp2(TOP - bound_exp)).astype(jnp.float16).reshape(size, rows // size, cols)
    side = side_rows(losses, bound_exp, cols)
    fill = -(rows // size) % EXTRA
    body = jnp.pad(body, ((0, 0), (0, fill), (0, 0)))
    return jnp.concatenate([body, jnp.broadcast_to(side[None], (size, *side.shape))], axis=1)


def unpacked(got, rows):
    side = got[:, -EXTRA, :].astype(jnp.float32)
    bound_exp = side[:, 2 * NBINS]
    loss_exp = side[:, 3 * NBINS]
    scale = jnp.exp2(bound_exp - TOP)
    losses = jnp.sum(
        (side[:, :NBINS] + side[:, NBINS : 2 * NBINS] * (1.0 / 1024.0)) * jnp.exp2(loss_exp - TOP)[:, None],
        axis=0,
    )
    total = jnp.sum(got[:, :rows, :].astype(jnp.float32) * scale[:, None, None], axis=0)
    return total, losses, jnp.sum(jnp.exp2(bound_exp))


def shards(attn, w_out, resid, target, gate, bins):
    samples = bins.shape[0]
    tok_rows, half = attn.shape
    per_sample = tok_rows // samples
    full_width = w_out.shape[1]
    own_cols = resid.shape[1]
    bin_ids = jnp.arange(NBINS, dtype=jnp.int32)
    one_hot = (bins[:, None] == bin_ids[None, :]).astype(jnp.float32)
    weights = bin_weights()
    me = lax.axis_index("mp")

    w_mine = lax.dynamic_slice_in_dim(w_out, me * own_cols, own_cols, axis=1)
    w_theirs = lax.dynamic_slice_in_dim(w_out, (1 - me) * own_cols, own_cols, axis=1)
    attn_other = partner(attn)
    w_other = partner(w_theirs)

    counts = summed_everywhere(jnp.sum(one_hot, axis=0)[None], DP[:2])
    counts = summed_everywhere(counts, DP[2])[0]
    floored = jnp.maximum(counts, 1.0)

    first = me == 0
    whole_attn = jnp.concatenate(
        [jnp.where(first, attn, attn_other), jnp.where(first, attn_other, attn)], axis=1
    )
    w_cols = jnp.concatenate(
        [jnp.where(first, w_mine, w_other), jnp.where(first, w_other, w_mine)], axis=0
    )
    projected = jnp.dot(whole_attn, w_cols, preferred_element_type=jnp.float32)
    proj_cube = projected.reshape(samples, per_sample, own_cols)
    hidden = (
        resid.reshape(samples, per_sample, own_cols).astype(jnp.float32)
        + gate[:, None, :] * proj_cube
    )
    error_cube = hidden - target.reshape(samples, per_sample, own_cols).astype(jnp.float32)
    sample_error = jnp.sum(error_cube * error_cube, axis=(1, 2)) / (per_sample * full_width)
    error_proj = jnp.sum(error_cube * proj_cube, axis=1)
    losses = jnp.sum(one_hot * sample_error[:, None], axis=0)
    losses = losses + partner(losses)

    scale_bin = LOSS_SCALE * weights / floored
    coefficient = jnp.sum(one_hot * scale_bin[None, :], axis=1) * (2.0 / (per_sample * full_width))
    grad_gate = coefficient[:, None] * error_proj
    d_exact = coefficient[:, None, None] * error_cube * gate[:, None, :]
    bound = ATTN_BOUND * jnp.max(jnp.sum(jnp.abs(d_exact), axis=(0, 1))) * 1.01
    d_proj = d_exact.astype(jnp.bfloat16).reshape(tok_rows, own_cols)
    total = lax.dot_general(
        whole_attn, d_proj, (((0,), (0,)), ((), ())), preferred_element_type=jnp.float32
    )
    for axis in DP:
        size = lax.axis_size(axis)
        rows = total.shape[0] // size
        got = lax.all_to_all(packed(total, losses, bound, size), axis, 0, 0, tiled=True)
        total, losses, bound = unpacked(got, rows)
    bin_loss = weights * losses / floored
    return (total, grad_gate, bin_loss)


def solution(mesh):
    finer = Mesh(mesh.devices.reshape(4, 8, 12, mesh.shape["mp"]), ("dp_0", "dp_1", "dp_2", "mp"))
    placed = (P(DP, "mp"), P("mp", None), P(DP, "mp"), P(DP, "mp"), P(DP, "mp"), P(DP))
    return jax.shard_map(
        shards,
        mesh=finer,
        in_specs=placed,
        out_specs=(P(DP, "mp"), P(DP, "mp"), P()),
        check_vma=False,
    )
```

```python
import math

import jax
import jax.numpy as jnp
from jax import lax
from jax.sharding import Mesh
from jax.sharding import PartitionSpec as P

NBINS = 128
X, YH, YL, ZH, ZL = "dp_x", "dp_yh", "dp_yl", "dp_zh", "dp_zl"
DP = (X, YH, YL, ZH, ZL)
NEAR = (X, YL, ZL)
FAR = (YH, ZH)
LOSS_SCALE = 4096.0
ATTN_BOUND = 6.0
TOP = 14.0
SIDE = 8
LOW = 1024.0


def bin_weights():
    centre = (jnp.arange(NBINS).astype(jnp.float32) + 0.5) / NBINS
    logit = jnp.log(centre) - jnp.log(1.0 - centre)
    return jnp.exp(-0.5 * logit * logit) / (math.sqrt(2.0 * math.pi) * centre * (1.0 - centre))


def group(axes):
    return math.prod(lax.axis_size(a) for a in axes)


def partner(x):
    return lax.ppermute(x, "mp", [(0, 1), (1, 0)])


def exchange(x, axes):
    return lax.all_to_all(x, axes, 0, 0, tiled=True)


def summed_everywhere(x, axes):
    spread = jnp.broadcast_to(x[None], (group(axes), *x.shape))
    return jnp.sum(exchange(spread, axes), axis=0)


def exponent_of(bound):
    return jnp.floor(jnp.log2(jnp.maximum(bound, 1e-30))) + 2.0


def halves(scaled):
    high = lax.reduce_precision(scaled, 5, 10)
    return high, (scaled - high) * LOW


def by_chunk(attn):
    tokens, feats = attn.shape
    yh, yl, zh, zl = (lax.axis_size(a) for a in (YH, YL, ZH, ZL))
    xs = lax.axis_size(X) // lax.axis_size("mp")
    last = feats // (xs * yh * yl * zh * zl)
    rows = attn.T.reshape(xs, yh, yl, zh, zl, last, tokens).transpose(0, 2, 4, 1, 3, 5, 6)
    rows = rows.reshape(xs * yl * zl, yh * zh * last, tokens)
    return jnp.pad(rows, ((0, 0), (0, SIDE), (0, 0))).reshape(-1, tokens)


def shards(attn, w_out, resid, target, gate, bins):
    samples = bins.shape[0]
    tok_rows, half = attn.shape
    per_sample = tok_rows // samples
    full_width = w_out.shape[1]
    own_cols = resid.shape[1]
    bin_ids = jnp.arange(NBINS, dtype=jnp.int32)
    one_hot = (bins[:, None] == bin_ids[None, :]).astype(jnp.float32)
    weights = bin_weights()
    me = lax.axis_index("mp")
    norm = per_sample * full_width

    counts = summed_everywhere(jnp.sum(one_hot, axis=0)[None], (X, YH, YL))
    counts = summed_everywhere(counts, (ZH, ZL))[0]
    floored = jnp.maximum(counts, 1.0)

    w_mine = lax.dynamic_slice_in_dim(w_out, me * own_cols, own_cols, axis=1)
    w_theirs = lax.dynamic_slice_in_dim(w_out, (1 - me) * own_cols, own_cols, axis=1)
    other = partner(jnp.concatenate([w_theirs, attn], axis=0))
    w_other, attn_other = other[:half], other[half:]
    projected = jnp.dot(attn, w_mine, preferred_element_type=jnp.float32) + jnp.dot(
        attn_other, w_other, preferred_element_type=jnp.float32
    )
    proj_cube = projected.reshape(samples, per_sample, own_cols)
    hidden = (
        resid.reshape(samples, per_sample, own_cols).astype(jnp.float32)
        + gate[:, None, :] * proj_cube
    )
    error_cube = hidden - target.reshape(samples, per_sample, own_cols).astype(jnp.float32)
    sample_error = jnp.sum(error_cube * error_cube, axis=(1, 2)) / norm
    error_proj = jnp.sum(error_cube * proj_cube, axis=1)
    losses = jnp.sum(one_hot * sample_error[:, None], axis=0)
    losses = losses + partner(losses)
    largest = jnp.sum(one_hot * (LOSS_SCALE * weights)[None, :], axis=1) * (2.0 / norm)
    reach = jnp.sum(largest[:, None] * jnp.sum(jnp.abs(error_cube * gate[:, None, :]), axis=1), axis=0)
    grad_exp = exponent_of(1.01 * ATTN_BOUND * jnp.max(reach))
    loss_exp = exponent_of(losses)
    high, low = halves(losses * jnp.exp2(TOP - loss_exp))

    first = me == 0
    own_rows, other_rows = by_chunk(attn), by_chunk(attn_other)
    features = jnp.concatenate(
        [jnp.where(first, own_rows, other_rows), jnp.where(first, other_rows, own_rows)], axis=0
    )
    widen = lambda row: jnp.pad(row, (0, own_cols - NBINS))
    side = [widen(high), widen(low), jnp.broadcast_to(grad_exp, (own_cols,)), widen(loss_exp)]
    near, far = group(NEAR), group(FAR)
    chunk = features.shape[0] // near
    keep = chunk - SIDE
    place = lax.broadcasted_iota(jnp.int32, (features.shape[0], 1), 0) % chunk

    scale_bin = LOSS_SCALE * weights / floored
    coefficient = jnp.sum(one_hot * scale_bin[None, :], axis=1) * (2.0 / norm)
    d_proj = (coefficient[:, None, None] * error_cube * gate[:, None, :]).astype(jnp.bfloat16)
    partial = jnp.dot(features, d_proj.reshape(tok_rows, own_cols), preferred_element_type=jnp.float32)
    partial = partial * jnp.exp2(TOP - grad_exp)
    for n, row in enumerate(side):
        partial = jnp.where(place == keep + n, row[None, :], partial)
    got = exchange(partial.astype(jnp.float16).reshape(near, chunk, own_cols), NEAR)

    sides = got[:, keep : keep + 4, :].astype(jnp.float32)
    grad_exp = jnp.max(sides[:, 2], axis=0) + math.log2(near)
    scale = jnp.exp2(sides[:, 2] - grad_exp)
    total = jnp.sum(got[:, :keep].astype(jnp.float32) * scale[:, None, :], axis=0)
    sides = sides[:, :, :NBINS]
    loss_exp = jnp.max(sides[:, 3], axis=0) + math.log2(near)
    high, low = halves(
        jnp.sum((sides[:, 0] + sides[:, 1] * (1.0 / LOW)) * jnp.exp2(sides[:, 3] - loss_exp), axis=0)
    )
    side = jnp.stack([high, low, grad_exp[:NBINS], loss_exp])
    side = jnp.pad(side, ((0, SIDE - 4), (0, 0))).astype(jnp.float16)
    body = total.astype(jnp.float16).reshape(far, -1, NBINS)
    keep = body.shape[1]
    body = jnp.concatenate([body, jnp.broadcast_to(side[None], (far, *side.shape))], axis=1)
    got = exchange(body, FAR).astype(jnp.float32)

    sides = got[:, keep : keep + 4]
    total = jnp.sum(got[:, :keep] * jnp.exp2(sides[:, 2:3] - TOP), axis=0)
    losses = jnp.sum((sides[:, 0] + sides[:, 1] * (1.0 / LOW)) * jnp.exp2(sides[:, 3] - TOP), axis=0)
    grad_gate = coefficient[:, None] * error_proj
    return (total.reshape(-1, own_cols), grad_gate, weights * losses / floored)


def solution(mesh):
    finer = Mesh(mesh.devices.reshape(4, 4, 2, 6, 2, mesh.shape["mp"]), (*DP, "mp"))
    placed = (P(DP, "mp"), P("mp", None), P(DP, "mp"), P(DP, "mp"), P(DP, "mp"), P(DP))
    return jax.shard_map(
        shards,
        mesh=finer,
        in_specs=placed,
        out_specs=(P(DP, "mp"), P(DP, "mp"), P()),
        check_vma=False,
    )
```

```python
import math

import jax
import jax.numpy as jnp
from jax import lax
from jax.experimental import pallas as pl
from jax.experimental.pallas import tpu as pltpu
from jax.sharding import Mesh
from jax.sharding import PartitionSpec as P

NBINS = 128
X, YH, YL, ZH, ZL = "dp_x", "dp_yh", "dp_yl", "dp_zh", "dp_zl"
DP = (X, YH, YL, ZH, ZL)
NEAR = (X, YL, ZL)
FAR = (YH, ZH)
LOSS_SCALE = 4096.0
ATTN_BOUND = 6.0
TOP = 14.0
SIDE = 8
LOW = 1024.0


def bin_weights():
    return weights_at(jnp.arange(NBINS).astype(jnp.float32))


def weights_at(index):
    centre = (index + 0.5) / NBINS
    logit = jnp.log(centre) - jnp.log(1.0 - centre)
    return jnp.exp(-0.5 * logit * logit) / (math.sqrt(2.0 * math.pi) * centre * (1.0 - centre))


def group(axes):
    return math.prod(lax.axis_size(a) for a in axes)


def partner(x):
    return lax.ppermute(x, "mp", [(0, 1), (1, 0)])


def exchange(x, axes):
    return lax.all_to_all(x, axes, 0, 0, tiled=True)


def summed_everywhere(x, axes):
    spread = jnp.broadcast_to(x[None], (group(axes), *x.shape))
    return jnp.sum(exchange(spread, axes), axis=0)


def exponent_of(bound):
    return jnp.floor(jnp.log2(jnp.maximum(bound, 1e-30))) + 2.0


def halves(scaled):
    high = lax.reduce_precision(scaled, 5, 10)
    return high, (scaled - high) * LOW


def forward_kernel(
    me, bins, attn, other, part, resid, target, gate, error, features, error_proj, losses, grad_exp
):
    tokens, half = attn.shape
    samples = gate.shape[0]
    per_sample = tokens // samples
    run = half // 2
    row = lax.broadcasted_iota(jnp.int32, (run, run), 0)
    piece = (row * 683) >> 16
    inner = row - 96 * piece
    quad = inner >> 2
    y_high = (quad * 43) >> 8
    z_high = quad - 6 * y_high
    source = y_high * 96 + (piece >> 1) * 48 + z_high * 8 + (piece & 1) * 4 + (inner & 3)
    picks = (source == lax.broadcasted_iota(jnp.int32, (run, run), 1)).astype(jnp.bfloat16)
    own, far = me[0] * half, (1 - me[0]) * half
    for first, block in ((own, attn), (far, other.at[half:, :])):
        for n in range(2):
            moved = lax.dot_general(
                picks,
                block[:, n * run : (n + 1) * run],
                (((1,), (1,)), ((), ())),
                preferred_element_type=jnp.float32,
            )
            features[pl.ds(pl.multiple_of(first + n * run, run), run), :] = moved.astype(jnp.bfloat16)

    lane = lax.broadcasted_iota(jnp.int32, (1, NBINS), 1)
    steepest = weights_at(lane.astype(jnp.float32)) * (LOSS_SCALE / (per_sample * half))
    found = jnp.zeros((1, NBINS), jnp.float32)
    reach = jnp.zeros((1, half), jnp.float32)
    for s in range(samples):
        rows = slice(s * per_sample, (s + 1) * per_sample)
        projected = part[rows, :] + jnp.dot(
            other[half + s * per_sample : half + (s + 1) * per_sample, :],
            other[:half, :],
            preferred_element_type=jnp.float32,
        )
        scale = gate[s : s + 1, :]
        diff = resid[rows, :].astype(jnp.float32) + scale * projected - target[rows, :].astype(jnp.float32)
        error[rows, :] = diff
        error_proj[s : s + 1, :] = jnp.sum(diff * projected, axis=0, keepdims=True)
        mine = lane == bins[s]
        largest = jnp.sum(jnp.where(mine, steepest, 0.0), axis=1, keepdims=True)
        reach = reach + largest * jnp.sum(jnp.abs(diff * scale), axis=0, keepdims=True)
        squares = jnp.sum(jnp.sum(diff * diff, axis=0, keepdims=True), axis=1, keepdims=True)
        found = found + jnp.where(mine, squares * (1.0 / (per_sample * 2 * half)), 0.0)
    losses[...] = found
    bound = jnp.max(reach, axis=1, keepdims=True) * (1.01 * ATTN_BOUND)
    grad_exp[...] = jnp.broadcast_to(exponent_of(bound), (1, NBINS))


def forward(me, bins, attn, other, part, resid, target, gate):
    tokens, half = attn.shape
    vmem, smem = pl.BlockSpec(memory_space=pltpu.VMEM), pl.BlockSpec(memory_space=pltpu.SMEM)
    return pl.pallas_call(
        forward_kernel,
        out_shape=(
            jax.ShapeDtypeStruct((tokens, half), jnp.float32),
            jax.ShapeDtypeStruct((2 * half, tokens), jnp.bfloat16),
            jax.ShapeDtypeStruct(gate.shape, jnp.float32),
            jax.ShapeDtypeStruct((1, NBINS), jnp.float32),
            jax.ShapeDtypeStruct((1, NBINS), jnp.float32),
        ),
        in_specs=[smem] * 2 + [vmem] * 6,
        out_specs=(vmem,) * 5,
        cost_estimate=pl.CostEstimate(flops=2 * 10**9, bytes_accessed=8 * 10**6, transcendentals=0),
        compiler_params=pltpu.CompilerParams(vmem_limit_bytes=20 * 2**20),
        name="forward",
    )(me, bins, attn, other, part, resid, target, gate)


def body(attn, w_out, resid, target, gate, bins):
    samples = bins.shape[0]
    tok_rows, _ = attn.shape
    per_sample = tok_rows // samples
    full_width = w_out.shape[1]
    own_cols = resid.shape[1]
    bin_ids = jnp.arange(NBINS, dtype=jnp.int32)
    one_hot = (bins[:, None] == bin_ids[None, :]).astype(jnp.float32)
    weights = bin_weights()
    me = lax.axis_index("mp")
    norm = per_sample * full_width

    counts = summed_everywhere(jnp.sum(one_hot, axis=0)[None], (X, YH, YL))
    counts = summed_everywhere(counts, (ZH, ZL))[0]
    floored = jnp.maximum(counts, 1.0)

    w_mine = lax.dynamic_slice_in_dim(w_out, me * own_cols, own_cols, axis=1)
    w_theirs = lax.dynamic_slice_in_dim(w_out, (1 - me) * own_cols, own_cols, axis=1)
    other = partner(jnp.concatenate([w_theirs, attn], axis=0))
    part = jnp.dot(attn, w_mine, preferred_element_type=jnp.float32)
    error, features, error_proj, losses, grad_exp = forward(
        me.reshape(1), bins, attn, other, part, resid, target, gate
    )
    error_cube = error.reshape(samples, per_sample, own_cols)
    losses, grad_exp = losses[0], grad_exp[0]
    losses = losses + partner(losses)
    loss_exp = exponent_of(losses)
    high, low = halves(losses * jnp.exp2(TOP - loss_exp))
    widen = lambda rows: jnp.pad(rows, ((0, SIDE - 4), (0, own_cols - NBINS)))
    side = widen(jnp.stack([high, low, grad_exp, loss_exp])).astype(jnp.float16)
    near, far = group(NEAR), group(FAR)

    scale_bin = LOSS_SCALE * weights / floored
    coefficient = jnp.sum(one_hot * scale_bin[None, :], axis=1) * (2.0 / norm)
    d_proj = (coefficient[:, None, None] * error_cube * gate[:, None, :]).astype(jnp.bfloat16)
    partial = jnp.dot(features, d_proj.reshape(tok_rows, own_cols), preferred_element_type=jnp.float32)
    grad_row = jnp.tile(jnp.exp2(TOP - grad_exp), own_cols // NBINS)
    partial = (partial * grad_row[None, :]).astype(jnp.float16).reshape(near, -1, own_cols)
    keep = partial.shape[1]
    partial = jnp.concatenate([partial, jnp.broadcast_to(side[None], (near, *side.shape))], axis=1)
    got = exchange(partial, NEAR)

    sides = got[:, keep : keep + 4, :NBINS].astype(jnp.float32)
    grad_exp = jnp.max(sides[:, 2], axis=0) + math.log2(near)
    scale = jnp.tile(jnp.exp2(sides[:, 2] - grad_exp), (1, own_cols // NBINS))
    total = jnp.sum(got[:, :keep].astype(jnp.float32) * scale[:, None, :], axis=0)
    loss_exp = jnp.max(sides[:, 3], axis=0) + math.log2(near)
    high, low = halves(
        jnp.sum((sides[:, 0] + sides[:, 1] * (1.0 / LOW)) * jnp.exp2(sides[:, 3] - loss_exp), axis=0)
    )
    side = jnp.stack([high, low, grad_exp, loss_exp])
    side = jnp.pad(side, ((0, SIDE - 4), (0, 0))).astype(jnp.float16)
    rows = total.astype(jnp.float16).reshape(far, -1, NBINS)
    keep = rows.shape[1]
    rows = jnp.concatenate([rows, jnp.broadcast_to(side[None], (far, *side.shape))], axis=1)
    got = exchange(rows, FAR).astype(jnp.float32)

    sides = got[:, keep : keep + 4]
    total = jnp.sum(got[:, :keep] * jnp.exp2(sides[:, 2:3] - TOP), axis=0)
    losses = jnp.sum((sides[:, 0] + sides[:, 1] * (1.0 / LOW)) * jnp.exp2(sides[:, 3] - TOP), axis=0)
    grad_gate = coefficient[:, None] * error_proj
    return (total.reshape(-1, own_cols), grad_gate, weights * losses / floored)


def solution(mesh):
    finer = Mesh(mesh.devices.reshape(4, 4, 2, 6, 2, mesh.shape["mp"]), (*DP, "mp"))
    placed = (P(DP, "mp"), P("mp", None), P(DP, "mp"), P(DP, "mp"), P(DP, "mp"), P(DP))
    return jax.shard_map(
        body,
        mesh=finer,
        in_specs=placed,
        out_specs=(P(DP, "mp"), P(DP, "mp"), P()),
        check_vma=False,
    )
```

```python
import math

import jax
import jax.numpy as jnp
from jax import lax
from jax.experimental import pallas as pl
from jax.experimental.pallas import tpu as pltpu
from jax.sharding import Mesh
from jax.sharding import PartitionSpec as P

NBINS = 128
X, YH, YL, ZH, ZL = "dp_x", "dp_yh", "dp_yl", "dp_zh", "dp_zl"
DP = (X, YH, YL, ZH, ZL)
NEAR = (X, YL, ZL)
FAR = (YH, ZH)
LOSS_SCALE = 4096.0
ATTN_BOUND = 6.0
TOP = 14.0
SIDE = 8
LOW = 1024.0


def weights_at(index):
    centre = (index + 0.5) / NBINS
    logit = jnp.log(centre) - jnp.log(1.0 - centre)
    return jnp.exp(-0.5 * logit * logit) / (math.sqrt(2.0 * math.pi) * centre * (1.0 - centre))


def group(axes):
    return math.prod(lax.axis_size(a) for a in axes)


def partner(x):
    return lax.ppermute(x, "mp", [(0, 1), (1, 0)])


def exchange(x, axes):
    return lax.all_to_all(x, axes, 0, 0, tiled=True)


def exponent_of(bound):
    return jnp.floor(jnp.log2(jnp.maximum(bound, 1e-30))) + 2.0


def halves(scaled):
    high = lax.reduce_precision(scaled, 5, 10)
    return high, (scaled - high) * LOW


VMEM = pl.BlockSpec(memory_space=pltpu.VMEM)
SMEM = pl.BlockSpec(memory_space=pltpu.SMEM)
HBM = pl.BlockSpec(memory_space=pltpu.HBM)


def grant(mib):
    return pltpu.CompilerParams(vmem_limit_bytes=mib * 2**20)


def bin_lanes():
    return lax.broadcasted_iota(jnp.int32, (1, NBINS), 1)


def count_kernel(bins, spread):
    lane = bin_lanes()
    found = jnp.zeros((1, NBINS), jnp.float32)
    for s in range(bins.shape[0]):
        found = found + (lane == bins[s]).astype(jnp.float32)
    spread[...] = jnp.broadcast_to(found[None], spread.shape)


def fold_kernel(got, spread):
    spread[...] = jnp.broadcast_to(jnp.sum(got[...], axis=0, keepdims=True), spread.shape)


def count_sweep(bins):
    plane, column = (X, YH, YL), (ZH, ZL)
    spread = pl.pallas_call(
        count_kernel,
        out_shape=jax.ShapeDtypeStruct((group(plane), 1, NBINS), jnp.float32),
        in_specs=[SMEM],
        out_specs=VMEM,
        name="count",
    )(bins)
    got = exchange(spread, plane)
    spread = pl.pallas_call(
        fold_kernel,
        out_shape=jax.ShapeDtypeStruct((group(column), 1, NBINS), jnp.float32),
        in_specs=[VMEM],
        out_specs=VMEM,
        compiler_params=grant(2),
        name="fold",
    )(got)
    return exchange(spread, column)


def feature_rows(block, picks):
    run = picks.shape[0]
    for n in range(block.shape[1] // run):
        yield lax.dot_general(
            picks,
            block[:, n * run : (n + 1) * run],
            (((1,), (1,)), ((), ())),
            preferred_element_type=jnp.float32,
        ).astype(jnp.bfloat16)


def row_picks(run):
    row = lax.broadcasted_iota(jnp.int32, (run, run), 0)
    piece = (row * 683) >> 16
    inner = row - 96 * piece
    quad = inner >> 2
    y_high = (quad * 43) >> 8
    z_high = quad - 6 * y_high
    source = y_high * 96 + (piece >> 1) * 48 + z_high * 8 + (piece & 1) * 4 + (inner & 3)
    return (source == lax.broadcasted_iota(jnp.int32, (run, run), 1)).astype(jnp.bfloat16)


def forward_kernel(
    me,
    bins,
    attn_hbm,
    other_hbm,
    part_hbm,
    resid_hbm,
    target_hbm,
    gate,
    error,
    features_hbm,
    error_proj,
    losses,
    grad_exp,
    grad_scale,
    attn,
    other,
    part,
    resid,
    target,
    features,
    sems,
):
    tokens, half = part.shape
    samples = gate.shape[0]
    per_sample = tokens // samples
    run = half // 2
    loads = [
        pltpu.make_async_copy(src, dst, sems.at[n])
        for n, (src, dst) in enumerate(
            (
                (attn_hbm, attn),
                (other_hbm, other),
                (part_hbm, part),
                (resid_hbm, resid),
                (target_hbm, target),
            )
        )
    ]
    for load in loads:
        load.start()
    picks = row_picks(run)
    mine = pl.multiple_of(me[0] * half, half)
    theirs = pl.multiple_of((1 - me[0]) * half, half)
    stores = []
    for first, block, load in ((mine, attn, loads[0]), (theirs, other.at[half:, :], loads[1])):
        load.wait()
        for n, moved in enumerate(feature_rows(block, picks)):
            features[pl.ds(pl.multiple_of(first + n * run, run), run), :] = moved
        rows = pl.ds(first, half)
        stores.append(pltpu.make_async_copy(features.at[rows, :], features_hbm.at[rows, :], sems.at[len(loads) + len(stores)]))
        stores[-1].start()
    for load in loads[2:]:
        load.wait()

    lane = bin_lanes()
    steepest = weights_at(lane.astype(jnp.float32)) * (LOSS_SCALE / (per_sample * half))
    found = jnp.zeros((1, NBINS), jnp.float32)
    reach = jnp.zeros((1, half), jnp.float32)
    for s in range(samples):
        rows = slice(s * per_sample, (s + 1) * per_sample)
        projected = part[rows, :] + jnp.dot(
            other[half + s * per_sample : half + (s + 1) * per_sample, :],
            other[:half, :],
            preferred_element_type=jnp.float32,
        )
        scale = gate[s : s + 1, :]
        diff = resid[rows, :].astype(jnp.float32) + scale * projected - target[rows, :].astype(jnp.float32)
        error[rows, :] = diff
        error_proj[s : s + 1, :] = jnp.sum(diff * projected, axis=0, keepdims=True)
        hit = lane == bins[s]
        largest = jnp.sum(jnp.where(hit, steepest, 0.0), axis=1, keepdims=True)
        reach = reach + largest * jnp.sum(jnp.abs(diff * scale), axis=0, keepdims=True)
        squares = jnp.sum(jnp.sum(diff * diff, axis=0, keepdims=True), axis=1, keepdims=True)
        found = found + jnp.where(hit, squares * (1.0 / (per_sample * 2 * half)), 0.0)
    losses[...] = found
    bound = exponent_of(jnp.max(reach, axis=1, keepdims=True) * (1.01 * ATTN_BOUND))
    grad_exp[...] = jnp.broadcast_to(bound, grad_exp.shape)
    grad_scale[...] = jnp.broadcast_to(jnp.exp2(TOP - bound), grad_scale.shape)
    for store in stores:
        store.wait()


def forward(me, bins, attn, other, part, resid, target, gate):
    tokens, half = part.shape
    operands = (attn, other, part, resid, target)
    return pl.pallas_call(
        forward_kernel,
        out_shape=(
            jax.ShapeDtypeStruct((tokens, half), jnp.float32),
            jax.ShapeDtypeStruct((2 * half, tokens), jnp.bfloat16),
            jax.ShapeDtypeStruct(gate.shape, jnp.float32),
            jax.ShapeDtypeStruct((1, NBINS), jnp.float32),
            jax.ShapeDtypeStruct((1, NBINS), jnp.float32),
            jax.ShapeDtypeStruct((1, half), jnp.float32),
        ),
        in_specs=[SMEM] * 2 + [HBM] * 5 + [VMEM],
        out_specs=(VMEM, HBM, VMEM, VMEM, VMEM, VMEM),
        scratch_shapes=[
            *(pltpu.VMEM(x.shape, x.dtype) for x in operands),
            pltpu.VMEM((2 * half, tokens), jnp.bfloat16),
            pltpu.SemaphoreType.DMA((len(operands) + 2,)),
        ],
        cost_estimate=pl.CostEstimate(flops=10**9, bytes_accessed=6 * 10**6, transcendentals=0),
        name="forward",
    )(me, bins, *operands, gate)


def scale_kernel(
    bins, got, losses, other_losses, grad_exp, error, gate, d_proj, steepness, per_count, side
):
    tokens, half = error.shape
    samples = gate.shape[0]
    per_sample = tokens // samples
    lane = bin_lanes()
    floored = jnp.maximum(jnp.sum(got[...], axis=0), 1.0)
    slope = weights_at(lane.astype(jnp.float32)) / floored
    per_count[...] = slope
    for s in range(samples):
        rows = slice(s * per_sample, (s + 1) * per_sample)
        coefficient = jnp.sum(jnp.where(lane == bins[s], slope * LOSS_SCALE, 0.0), axis=1, keepdims=True)
        coefficient = coefficient * (1.0 / (per_sample * half))
        d_proj[rows, :] = (coefficient * error[rows, :] * gate[s : s + 1, :]).astype(jnp.bfloat16)
        steepness[s : s + 1, :] = jnp.broadcast_to(coefficient, (1, NBINS))
    total = losses[...] + other_losses[...]
    loss_exp = exponent_of(total)
    high, low = halves(total * jnp.exp2(TOP - loss_exp))
    side[...] = jnp.zeros(side.shape, jnp.float32)
    for n, row in enumerate((high, low, grad_exp[...], loss_exp)):
        side[n : n + 1, :NBINS] = row


def scaled(bins, got, losses, other_losses, grad_exp, error, gate):
    return pl.pallas_call(
        scale_kernel,
        out_shape=(
            jax.ShapeDtypeStruct(error.shape, jnp.bfloat16),
            jax.ShapeDtypeStruct((gate.shape[0], NBINS), jnp.float32),
            jax.ShapeDtypeStruct((1, NBINS), jnp.float32),
            jax.ShapeDtypeStruct((SIDE, gate.shape[1]), jnp.float32),
        ),
        in_specs=[SMEM] + [VMEM] * 6,
        out_specs=(VMEM,) * 4,
        cost_estimate=pl.CostEstimate(flops=10**7, bytes_accessed=2 * 10**6, transcendentals=0),
        compiler_params=grant(20),
        name="scaled",
    )(bins, got, losses, other_losses, grad_exp, error, gate)


def body(attn, w_out, resid, target, gate, bins):
    own_cols = resid.shape[1]
    me = lax.axis_index("mp")
    got = count_sweep(bins)
    w_mine = lax.dynamic_slice_in_dim(w_out, me * own_cols, own_cols, axis=1)
    w_theirs = lax.dynamic_slice_in_dim(w_out, (1 - me) * own_cols, own_cols, axis=1)
    other = partner(jnp.concatenate([w_theirs, attn], axis=0))
    part = jnp.dot(attn, w_mine, preferred_element_type=jnp.float32)
    error, features, error_proj, losses, grad_exp, grad_scale = forward(
        me.reshape(1), bins, attn, other, part, resid, target, gate
    )
    other_losses = partner(losses)
    near, far = group(NEAR), group(FAR)
    d_proj, steepness, per_count, side = scaled(bins, got, losses, other_losses, grad_exp, error, gate)
    side = side.astype(jnp.float16)
    partial = jnp.dot(features, d_proj, preferred_element_type=jnp.float32)
    partial = (partial * grad_scale).astype(jnp.float16).reshape(near, -1, own_cols)
    keep = partial.shape[1]
    partial = jnp.concatenate([partial, jnp.broadcast_to(side[None], (near, *side.shape))], axis=1)
    got = exchange(partial, NEAR)

    sides = got[:, keep : keep + 4, :NBINS].astype(jnp.float32)
    grad_exp = jnp.max(sides[:, 2], axis=0) + math.log2(near)
    scale = jnp.tile(jnp.exp2(sides[:, 2] - grad_exp), (1, own_cols // NBINS))
    total = jnp.sum(got[:, :keep].astype(jnp.float32) * scale[:, None, :], axis=0)
    loss_exp = jnp.max(sides[:, 3], axis=0) + math.log2(near)
    high, low = halves(
        jnp.sum((sides[:, 0] + sides[:, 1] * (1.0 / LOW)) * jnp.exp2(sides[:, 3] - loss_exp), axis=0)
    )
    side = jnp.stack([high, low, grad_exp, loss_exp])
    side = jnp.pad(side, ((0, SIDE - 4), (0, 0))).astype(jnp.float16)
    rows = total.astype(jnp.float16).reshape(far, -1, NBINS)
    keep = rows.shape[1]
    rows = jnp.concatenate([rows, jnp.broadcast_to(side[None], (far, *side.shape))], axis=1)
    got = exchange(rows, FAR).astype(jnp.float32)

    sides = got[:, keep : keep + 4]
    total = jnp.sum(got[:, :keep] * jnp.exp2(sides[:, 2:3] - TOP), axis=0)
    losses = jnp.sum((sides[:, 0] + sides[:, 1] * (1.0 / LOW)) * jnp.exp2(sides[:, 3] - TOP), axis=0)
    return (total.reshape(-1, own_cols), steepness[:, :1] * error_proj, per_count[0] * losses)


def solution(mesh):
    finer = Mesh(mesh.devices.reshape(4, 4, 2, 6, 2, mesh.shape["mp"]), (*DP, "mp"))
    placed = (P(DP, "mp"), P("mp", None), P(DP, "mp"), P(DP, "mp"), P(DP, "mp"), P(DP))
    return jax.shard_map(
        body,
        mesh=finer,
        in_specs=placed,
        out_specs=(P(DP, "mp"), P(DP, "mp"), P()),
        check_vma=False,
    )
```

```python
import math

import jax
import jax.numpy as jnp
from jax import lax
from jax.experimental import pallas as pl
from jax.experimental.pallas import tpu as pltpu
from jax.sharding import Mesh
from jax.sharding import PartitionSpec as P

NBINS = 128
X, YH, YL, ZH, ZL = "dp_x", "dp_yh", "dp_yl", "dp_zh", "dp_zl"
DP = (X, YH, YL, ZH, ZL)
NEAR = (X, YL, ZL)
FAR = (YH, ZH)
LOSS_SCALE = 4096.0
ATTN_BOUND = 6.0
TOP = 14.0
SIDE = 8
LOW = 1024.0


def weights_at(index):
    centre = (index + 0.5) / NBINS
    logit = jnp.log(centre) - jnp.log(1.0 - centre)
    return jnp.exp(-0.5 * logit * logit) / (math.sqrt(2.0 * math.pi) * centre * (1.0 - centre))


def group(axes):
    return math.prod(lax.axis_size(a) for a in axes)


def partner(x):
    return lax.ppermute(x, "mp", [(0, 1), (1, 0)])


def exchange(x, axes):
    return lax.all_to_all(x, axes, 0, 0, tiled=True)


def exponent_of(bound):
    return jnp.floor(jnp.log2(jnp.maximum(bound, 1e-30))) + 2.0


def halves(scaled):
    high = lax.reduce_precision(scaled, 5, 10)
    return high, (scaled - high) * LOW


VMEM = pl.BlockSpec(memory_space=pltpu.VMEM)
SMEM = pl.BlockSpec(memory_space=pltpu.SMEM)
HBM = pl.BlockSpec(memory_space=pltpu.HBM)


def grant(mib):
    return pltpu.CompilerParams(vmem_limit_bytes=mib * 2**20)


def bin_lanes():
    return lax.broadcasted_iota(jnp.int32, (1, NBINS), 1)


def count_kernel(bins, spread):
    lane = bin_lanes()
    found = jnp.zeros((1, NBINS), jnp.float32)
    for s in range(bins.shape[0]):
        found = found + (lane == bins[s]).astype(jnp.float32)
    spread[...] = jnp.broadcast_to(found[None], spread.shape)


def fold_kernel(got, spread):
    spread[...] = jnp.broadcast_to(jnp.sum(got[...], axis=0, keepdims=True), spread.shape)


def count_sweep(bins):
    plane, column = (X, YH, YL), (ZH, ZL)
    spread = pl.pallas_call(
        count_kernel,
        out_shape=jax.ShapeDtypeStruct((group(plane), 1, NBINS), jnp.float32),
        in_specs=[SMEM],
        out_specs=VMEM,
        name="count",
    )(bins)
    got = exchange(spread, plane)
    spread = pl.pallas_call(
        fold_kernel,
        out_shape=jax.ShapeDtypeStruct((group(column), 1, NBINS), jnp.float32),
        in_specs=[VMEM],
        out_specs=VMEM,
        compiler_params=grant(2),
        name="fold",
    )(got)
    return exchange(spread, column)


def feature_rows(block, picks):
    run = picks.shape[0]
    for n in range(block.shape[1] // run):
        yield lax.dot_general(
            picks,
            block[:, n * run : (n + 1) * run],
            (((1,), (1,)), ((), ())),
            preferred_element_type=jnp.float32,
        ).astype(jnp.bfloat16)


def row_picks(run):
    row = lax.broadcasted_iota(jnp.int32, (run, run), 0)
    piece = (row * 683) >> 16
    inner = row - 96 * piece
    quad = inner >> 2
    y_high = (quad * 43) >> 8
    z_high = quad - 6 * y_high
    source = y_high * 96 + (piece >> 1) * 48 + z_high * 8 + (piece & 1) * 4 + (inner & 3)
    return (source == lax.broadcasted_iota(jnp.int32, (run, run), 1)).astype(jnp.bfloat16)


def forward_kernel(
    me,
    bins,
    attn_hbm,
    other_hbm,
    part_hbm,
    resid_hbm,
    target_hbm,
    gate,
    error,
    features_hbm,
    error_proj,
    marks,
    attn,
    other,
    part,
    resid,
    target,
    features,
    sems,
):
    tokens, half = part.shape
    samples = gate.shape[0]
    per_sample = tokens // samples
    run = half // 2
    loads = [
        pltpu.make_async_copy(src, dst, sems.at[n])
        for n, (src, dst) in enumerate(
            (
                (attn_hbm, attn),
                (other_hbm, other),
                (part_hbm, part),
                (resid_hbm, resid),
                (target_hbm, target),
            )
        )
    ]
    for load in loads:
        load.start()
    picks = row_picks(run)
    mine = pl.multiple_of(me[0] * half, half)
    theirs = pl.multiple_of((1 - me[0]) * half, half)
    stores = []
    for first, block, load in ((mine, attn, loads[0]), (theirs, other.at[half:, :], loads[1])):
        load.wait()
        for n, moved in enumerate(feature_rows(block, picks)):
            features[pl.ds(pl.multiple_of(first + n * run, run), run), :] = moved
        rows = pl.ds(first, half)
        stores.append(pltpu.make_async_copy(features.at[rows, :], features_hbm.at[rows, :], sems.at[len(loads) + len(stores)]))
        stores[-1].start()
    for load in loads[2:]:
        load.wait()

    lane = bin_lanes()
    steepest = weights_at(lane.astype(jnp.float32)) * (LOSS_SCALE / (per_sample * half))
    found = jnp.zeros((1, NBINS), jnp.float32)
    reach = jnp.zeros((1, half), jnp.float32)
    for s in range(samples):
        rows = slice(s * per_sample, (s + 1) * per_sample)
        projected = part[rows, :] + jnp.dot(
            other[half + s * per_sample : half + (s + 1) * per_sample, :],
            other[:half, :],
            preferred_element_type=jnp.float32,
        )
        scale = gate[s : s + 1, :]
        diff = resid[rows, :].astype(jnp.float32) + scale * projected - target[rows, :].astype(jnp.float32)
        error[rows, :] = diff
        error_proj[s : s + 1, :] = jnp.sum(diff * projected, axis=0, keepdims=True)
        hit = lane == bins[s]
        largest = jnp.sum(jnp.where(hit, steepest, 0.0), axis=1, keepdims=True)
        reach = reach + largest * jnp.sum(jnp.abs(diff * scale), axis=0, keepdims=True)
        squares = jnp.sum(jnp.sum(diff * diff, axis=0, keepdims=True), axis=1, keepdims=True)
        found = found + jnp.where(hit, squares * (1.0 / (per_sample * 2 * half)), 0.0)
    bound = exponent_of(jnp.max(reach, axis=1, keepdims=True) * (1.01 * ATTN_BOUND))
    marks[...] = jnp.broadcast_to(bound, marks.shape)
    marks[:1, :] = found
    for store in stores:
        store.wait()


def forward(me, bins, attn, other, part, resid, target, gate):
    tokens, half = part.shape
    operands = (attn, other, part, resid, target)
    return pl.pallas_call(
        forward_kernel,
        out_shape=(
            jax.ShapeDtypeStruct((tokens, half), jnp.float32),
            jax.ShapeDtypeStruct((2 * half, tokens), jnp.bfloat16),
            jax.ShapeDtypeStruct(gate.shape, jnp.float32),
            jax.ShapeDtypeStruct((SIDE, NBINS), jnp.float32),
        ),
        in_specs=[SMEM] * 2 + [HBM] * 5 + [VMEM],
        out_specs=(VMEM, HBM, VMEM, VMEM),
        scratch_shapes=[
            *(pltpu.VMEM(x.shape, x.dtype) for x in operands),
            pltpu.VMEM((2 * half, tokens), jnp.bfloat16),
            pltpu.SemaphoreType.DMA((len(operands) + 2,)),
        ],
        cost_estimate=pl.CostEstimate(flops=10**9, bytes_accessed=6 * 10**6, transcendentals=0),
        name="forward",
    )(me, bins, *operands, gate)


def scale_kernel(
    bins,
    got_hbm,
    marks_hbm,
    other_hbm,
    gate_hbm,
    error_proj_hbm,
    error_hbm,
    d_proj,
    grad_gate,
    per_count,
    side,
    got,
    marks,
    other,
    gate,
    error_proj,
    error,
    sems,
):
    tokens, half = error.shape
    samples = gate.shape[0]
    per_sample = tokens // samples
    sample_rows = [slice(s * per_sample, (s + 1) * per_sample) for s in range(samples)]
    pairs = [(got_hbm, got), (marks_hbm, marks), (other_hbm, other), (gate_hbm, gate)]
    pairs += [(error_hbm.at[rows, :], error.at[rows, :]) for rows in sample_rows]
    pairs += [(error_proj_hbm, error_proj)]
    loads = [pltpu.make_async_copy(src, dst, sems.at[n]) for n, (src, dst) in enumerate(pairs)]
    for load in loads:
        load.start()
    lane = bin_lanes()
    weights = weights_at(lane.astype(jnp.float32))
    side[...] = jnp.zeros(side.shape, jnp.float32)
    for load in loads[:4]:
        load.wait()
    slope = weights / jnp.maximum(jnp.sum(got[...], axis=0), 1.0)
    per_count[...] = slope
    grad_exp = marks[1:2, :]
    lift = jnp.exp2(TOP - grad_exp[:, :1])
    coefficients = [
        jnp.sum(jnp.where(lane == bins[s], slope * LOSS_SCALE, 0.0), axis=1, keepdims=True)
        * (1.0 / (per_sample * half))
        for s in range(samples)
    ]
    total = marks[:1, :] + other[:1, :]
    loss_exp = exponent_of(total)
    high, low = halves(total * jnp.exp2(TOP - loss_exp))
    for n, row in enumerate((high, low, grad_exp, loss_exp)):
        side[n : n + 1, :NBINS] = row
    for s, rows in enumerate(sample_rows):
        loads[4 + s].wait()
        rounded = (coefficients[s] * error[rows, :] * gate[s : s + 1, :]).astype(jnp.bfloat16)
        d_proj[rows, :] = (rounded.astype(jnp.float32) * lift).astype(jnp.bfloat16)
    loads[-1].wait()
    for s in range(samples):
        grad_gate[s : s + 1, :] = coefficients[s] * error_proj[s : s + 1, :]


def scaled(bins, got, marks, other_marks, gate, error_proj, error):
    operands = (got, marks, other_marks, gate, error_proj, error)
    return pl.pallas_call(
        scale_kernel,
        out_shape=(
            jax.ShapeDtypeStruct(error.shape, jnp.bfloat16),
            jax.ShapeDtypeStruct(gate.shape, jnp.float32),
            jax.ShapeDtypeStruct((1, NBINS), jnp.float32),
            jax.ShapeDtypeStruct((SIDE, gate.shape[1]), jnp.float32),
        ),
        in_specs=[SMEM] + [HBM] * 6,
        out_specs=(VMEM,) * 4,
        scratch_shapes=[
            *(pltpu.VMEM(x.shape, x.dtype) for x in operands),
            pltpu.SemaphoreType.DMA((len(operands) - 1 + gate.shape[0],)),
        ],
        cost_estimate=pl.CostEstimate(flops=10**7, bytes_accessed=2 * 10**6, transcendentals=0),
        name="scaled",
    )(bins, *operands)


def body(attn, w_out, resid, target, gate, bins):
    own_cols = resid.shape[1]
    me = lax.axis_index("mp")
    got = count_sweep(bins)
    w_mine = lax.dynamic_slice_in_dim(w_out, me * own_cols, own_cols, axis=1)
    w_theirs = lax.dynamic_slice_in_dim(w_out, (1 - me) * own_cols, own_cols, axis=1)
    other = partner(jnp.concatenate([w_theirs, attn], axis=0))
    part = jnp.dot(attn, w_mine, preferred_element_type=jnp.float32)
    error, features, error_proj, marks = forward(me.reshape(1), bins, attn, other, part, resid, target, gate)
    other_marks = partner(marks)
    near, far = group(NEAR), group(FAR)
    d_proj, grad_gate, per_count, side = scaled(bins, got, marks, other_marks, gate, error_proj, error)
    side = side.astype(jnp.float16)
    partial = jnp.dot(features, d_proj, preferred_element_type=jnp.float32)
    partial = partial.astype(jnp.float16).reshape(near, -1, own_cols)
    keep = partial.shape[1]
    partial = jnp.concatenate([partial, jnp.broadcast_to(side[None], (near, *side.shape))], axis=1)
    got = exchange(partial, NEAR)

    sides = got[:, keep : keep + 4, :NBINS].astype(jnp.float32)
    grad_exp = jnp.max(sides[:, 2], axis=0) + math.log2(near)
    scale = jnp.tile(jnp.exp2(sides[:, 2] - grad_exp), (1, own_cols // NBINS))
    total = jnp.sum(got[:, :keep].astype(jnp.float32) * scale[:, None, :], axis=0)
    loss_exp = jnp.max(sides[:, 3], axis=0) + math.log2(near)
    high, low = halves(
        jnp.sum((sides[:, 0] + sides[:, 1] * (1.0 / LOW)) * jnp.exp2(sides[:, 3] - loss_exp), axis=0)
    )
    side = jnp.stack([high, low, grad_exp, loss_exp])
    side = jnp.pad(side, ((0, SIDE - 4), (0, 0))).astype(jnp.float16)
    rows = total.astype(jnp.float16).reshape(far, -1, NBINS)
    keep = rows.shape[1]
    rows = jnp.concatenate([rows, jnp.broadcast_to(side[None], (far, *side.shape))], axis=1)
    got = exchange(rows, FAR).astype(jnp.float32)

    sides = got[:, keep : keep + 4]
    total = jnp.sum(got[:, :keep] * jnp.exp2(sides[:, 2:3] - TOP), axis=0)
    losses = jnp.sum((sides[:, 0] + sides[:, 1] * (1.0 / LOW)) * jnp.exp2(sides[:, 3] - TOP), axis=0)
    return (total.reshape(-1, own_cols), grad_gate, per_count[0] * losses)


def solution(mesh):
    finer = Mesh(mesh.devices.reshape(4, 4, 2, 6, 2, mesh.shape["mp"]), (*DP, "mp"))
    placed = (P(DP, "mp"), P("mp", None), P(DP, "mp"), P(DP, "mp"), P(DP, "mp"), P(DP))
    return jax.shard_map(
        body,
        mesh=finer,
        in_specs=placed,
        out_specs=(P(DP, "mp"), P(DP, "mp"), P()),
        check_vma=False,
    )
```

```python
import math

import jax
import jax.numpy as jnp
from jax import lax
from jax.experimental import pallas as pl
from jax.experimental.pallas import tpu as pltpu
from jax.sharding import Mesh
from jax.sharding import PartitionSpec as P

NBINS = 128
X, YH, YL, ZH, ZL = "dp_x", "dp_yh", "dp_yl", "dp_zh", "dp_zl"
DP = (X, YH, YL, ZH, ZL)
NEAR = (X, YL, ZL)
FAR = (YH, ZH)
LOSS_SCALE = 4096.0
ATTN_BOUND = 6.0
TOP = 14.0
SIDE = 8
LOW = 1024.0


def weights_at(index):
    centre = (index + 0.5) / NBINS
    logit = jnp.log(centre) - jnp.log(1.0 - centre)
    return jnp.exp(-0.5 * logit * logit) / (math.sqrt(2.0 * math.pi) * centre * (1.0 - centre))


def group(axes):
    return math.prod(lax.axis_size(a) for a in axes)


def partner(x):
    return lax.ppermute(x, "mp", [(0, 1), (1, 0)])


def exchange(x, axes):
    return lax.all_to_all(x, axes, 0, 0, tiled=True)


def exponent_of(bound):
    return jnp.floor(jnp.log2(jnp.maximum(bound, 1e-30))) + 2.0


def halves(scaled):
    high = lax.reduce_precision(scaled, 5, 10)
    return high, (scaled - high) * LOW


VMEM = pl.BlockSpec(memory_space=pltpu.VMEM)
SMEM = pl.BlockSpec(memory_space=pltpu.SMEM)
HBM = pl.BlockSpec(memory_space=pltpu.HBM)


def grant(mib):
    return pltpu.CompilerParams(vmem_limit_bytes=mib * 2**20)


def bin_lanes():
    return lax.broadcasted_iota(jnp.int32, (1, NBINS), 1)


def count_kernel(bins, spread):
    lane = bin_lanes()
    found = jnp.zeros((1, NBINS), jnp.float32)
    for s in range(bins.shape[0]):
        found = found + (lane == bins[s]).astype(jnp.float32)
    spread[...] = jnp.broadcast_to(found[None], spread.shape)


def fold_kernel(got, spread):
    spread[...] = jnp.broadcast_to(jnp.sum(got[...], axis=0, keepdims=True), spread.shape)


def count_sweep(bins):
    plane, column = (X, YH, YL), (ZH, ZL)
    spread = pl.pallas_call(
        count_kernel,
        out_shape=jax.ShapeDtypeStruct((group(plane), 1, NBINS), jnp.float32),
        in_specs=[SMEM],
        out_specs=VMEM,
        name="count",
    )(bins)
    got = exchange(spread, plane)
    spread = pl.pallas_call(
        fold_kernel,
        out_shape=jax.ShapeDtypeStruct((group(column), 1, NBINS), jnp.float32),
        in_specs=[VMEM],
        out_specs=VMEM,
        compiler_params=grant(2),
        name="fold",
    )(got)
    return exchange(spread, column)


def feature_rows(block, picks):
    run = picks.shape[0]
    for n in range(block.shape[1] // run):
        yield lax.dot_general(
            picks,
            block[:, n * run : (n + 1) * run],
            (((1,), (1,)), ((), ())),
            preferred_element_type=jnp.float32,
        ).astype(jnp.bfloat16)


def row_picks(run):
    row = lax.broadcasted_iota(jnp.int32, (run, run), 0)
    piece = (row * 683) >> 16
    inner = row - 96 * piece
    quad = inner >> 2
    y_high = (quad * 43) >> 8
    z_high = quad - 6 * y_high
    source = y_high * 96 + (piece >> 1) * 48 + z_high * 8 + (piece & 1) * 4 + (inner & 3)
    return (source == lax.broadcasted_iota(jnp.int32, (run, run), 1)).astype(jnp.bfloat16)


def forward_kernel(
    me,
    bins,
    attn_hbm,
    other_hbm,
    w_hbm,
    resid_hbm,
    target_hbm,
    gate,
    error_hbm,
    features_hbm,
    error_proj,
    marks,
    attn,
    attn_far,
    w_near,
    w_far,
    resid,
    target,
    error,
    features,
    load_sems,
    store_sems,
):
    tokens, half = attn.shape
    samples = gate.shape[0]
    per_sample = tokens // samples
    run = half // 2
    mine = pl.multiple_of(me[0] * half, half)
    theirs = pl.multiple_of((1 - me[0]) * half, half)
    pairs = (
        (attn_hbm, attn),
        (other_hbm.at[half:, :], attn_far),
        (w_hbm.at[:, pl.ds(mine, half)], w_near),
        (other_hbm.at[:half, :], w_far),
        (resid_hbm, resid),
        (target_hbm, target),
    )
    loads = [pltpu.make_async_copy(src, dst, load_sems.at[n]) for n, (src, dst) in enumerate(pairs)]
    for load in loads:
        load.start()
    stores = []

    def store(src, dst, rows):
        stores.append(pltpu.make_async_copy(src.at[rows, :], dst.at[rows, :], store_sems.at[len(stores)]))
        stores[-1].start()

    picks = row_picks(run)
    for first, block, load in ((mine, attn, loads[0]), (theirs, attn_far, loads[1])):
        load.wait()
        for n, moved in enumerate(feature_rows(block, picks)):
            features[pl.ds(pl.multiple_of(first + n * run, run), run), :] = moved
        store(features, features_hbm, pl.ds(first, half))
    for load in loads[2:]:
        load.wait()

    lane = bin_lanes()
    steepest = weights_at(lane.astype(jnp.float32)) * (LOSS_SCALE / (per_sample * half))
    found = jnp.zeros((1, NBINS), jnp.float32)
    reach = jnp.zeros((1, half), jnp.float32)
    for s in range(samples):
        rows = slice(s * per_sample, (s + 1) * per_sample)
        projected = jnp.dot(attn[rows, :], w_near[...], preferred_element_type=jnp.float32) + jnp.dot(
            attn_far[rows, :], w_far[...], preferred_element_type=jnp.float32
        )
        scale = gate[s : s + 1, :]
        diff = resid[rows, :].astype(jnp.float32) + scale * projected - target[rows, :].astype(jnp.float32)
        error[rows, :] = diff
        store(error, error_hbm, pl.ds(s * per_sample, per_sample))
        error_proj[s : s + 1, :] = jnp.sum(diff * projected, axis=0, keepdims=True)
        hit = lane == bins[s]
        largest = jnp.sum(jnp.where(hit, steepest, 0.0), axis=1, keepdims=True)
        reach = reach + largest * jnp.sum(jnp.abs(diff * scale), axis=0, keepdims=True)
        squares = jnp.sum(jnp.sum(diff * diff, axis=0, keepdims=True), axis=1, keepdims=True)
        found = found + jnp.where(hit, squares * (1.0 / (per_sample * 2 * half)), 0.0)
    bound = exponent_of(jnp.max(reach, axis=1, keepdims=True) * (1.01 * ATTN_BOUND))
    marks[...] = jnp.broadcast_to(bound, marks.shape)
    marks[:1, :] = found
    for copy in stores:
        copy.wait()


def forward(me, bins, attn, other, w_out, resid, target, gate):
    tokens, half = attn.shape
    block = pltpu.VMEM(attn.shape, attn.dtype)
    square = pltpu.VMEM((half, half), attn.dtype)
    return pl.pallas_call(
        forward_kernel,
        out_shape=(
            jax.ShapeDtypeStruct((tokens, half), jnp.float32),
            jax.ShapeDtypeStruct((2 * half, tokens), jnp.bfloat16),
            jax.ShapeDtypeStruct(gate.shape, jnp.float32),
            jax.ShapeDtypeStruct((SIDE, NBINS), jnp.float32),
        ),
        in_specs=[SMEM] * 2 + [HBM] * 5 + [VMEM],
        out_specs=(HBM, HBM, VMEM, VMEM),
        scratch_shapes=[
            block,
            block,
            square,
            square,
            block,
            block,
            pltpu.VMEM((tokens, half), jnp.float32),
            pltpu.VMEM((2 * half, tokens), jnp.bfloat16),
            pltpu.SemaphoreType.DMA((6,)),
            pltpu.SemaphoreType.DMA((2 + gate.shape[0],)),
        ],
        cost_estimate=pl.CostEstimate(flops=10**9, bytes_accessed=6 * 10**6, transcendentals=0),
        compiler_params=grant(50),
        name="forward",
    )(me, bins, attn, other, w_out, resid, target, gate)


def scale_kernel(
    bins, got, marks, other_marks, error, gate, d_proj, steepness, per_count, side
):
    tokens, half = error.shape
    samples = gate.shape[0]
    per_sample = tokens // samples
    lane = bin_lanes()
    floored = jnp.maximum(jnp.sum(got[...], axis=0), 1.0)
    slope = weights_at(lane.astype(jnp.float32)) / floored
    per_count[...] = slope
    grad_exp = marks[1:2, :]
    lift = jnp.exp2(TOP - grad_exp[:, :1])
    for s in range(samples):
        rows = slice(s * per_sample, (s + 1) * per_sample)
        coefficient = jnp.sum(jnp.where(lane == bins[s], slope * LOSS_SCALE, 0.0), axis=1, keepdims=True)
        coefficient = coefficient * (1.0 / (per_sample * half))
        rounded = (coefficient * error[rows, :] * gate[s : s + 1, :]).astype(jnp.bfloat16)
        d_proj[rows, :] = (rounded.astype(jnp.float32) * lift).astype(jnp.bfloat16)
        steepness[s : s + 1, :] = jnp.broadcast_to(coefficient, (1, NBINS))
    total = marks[:1, :] + other_marks[:1, :]
    loss_exp = exponent_of(total)
    high, low = halves(total * jnp.exp2(TOP - loss_exp))
    side[...] = jnp.zeros(side.shape, jnp.float32)
    for n, row in enumerate((high, low, grad_exp, loss_exp)):
        side[n : n + 1, :NBINS] = row


def scaled(bins, got, marks, other_marks, error, gate):
    return pl.pallas_call(
        scale_kernel,
        out_shape=(
            jax.ShapeDtypeStruct(error.shape, jnp.bfloat16),
            jax.ShapeDtypeStruct((gate.shape[0], NBINS), jnp.float32),
            jax.ShapeDtypeStruct((1, NBINS), jnp.float32),
            jax.ShapeDtypeStruct((SIDE, gate.shape[1]), jnp.float32),
        ),
        in_specs=[SMEM] + [VMEM] * 5,
        out_specs=(VMEM,) * 4,
        cost_estimate=pl.CostEstimate(flops=10**7, bytes_accessed=2 * 10**6, transcendentals=0),
        compiler_params=grant(20),
        name="scaled",
    )(bins, got, marks, other_marks, error, gate)


def body(attn, w_out, resid, target, gate, bins):
    own_cols = resid.shape[1]
    me = lax.axis_index("mp")
    got = count_sweep(bins)
    w_theirs = lax.dynamic_slice_in_dim(w_out, (1 - me) * own_cols, own_cols, axis=1)
    other = partner(jnp.concatenate([w_theirs, attn], axis=0))
    error, features, error_proj, marks = forward(
        me.reshape(1), bins, attn, other, w_out, resid, target, gate
    )
    other_marks = partner(marks)
    near, far = group(NEAR), group(FAR)
    d_proj, steepness, per_count, side = scaled(bins, got, marks, other_marks, error, gate)
    side = side.astype(jnp.float16)
    partial = jnp.dot(features, d_proj, preferred_element_type=jnp.float32)
    partial = partial.astype(jnp.float16).reshape(near, -1, own_cols)
    keep = partial.shape[1]
    partial = jnp.concatenate([partial, jnp.broadcast_to(side[None], (near, *side.shape))], axis=1)
    got = exchange(partial, NEAR)

    sides = got[:, keep : keep + 4, :NBINS].astype(jnp.float32)
    grad_exp = jnp.max(sides[:, 2], axis=0) + math.log2(near)
    scale = jnp.tile(jnp.exp2(sides[:, 2] - grad_exp), (1, own_cols // NBINS))
    total = jnp.sum(got[:, :keep].astype(jnp.float32) * scale[:, None, :], axis=0)
    loss_exp = jnp.max(sides[:, 3], axis=0) + math.log2(near)
    high, low = halves(
        jnp.sum((sides[:, 0] + sides[:, 1] * (1.0 / LOW)) * jnp.exp2(sides[:, 3] - loss_exp), axis=0)
    )
    side = jnp.stack([high, low, grad_exp, loss_exp])
    side = jnp.pad(side, ((0, SIDE - 4), (0, 0))).astype(jnp.float16)
    rows = total.astype(jnp.float16).reshape(far, -1, NBINS)
    keep = rows.shape[1]
    rows = jnp.concatenate([rows, jnp.broadcast_to(side[None], (far, *side.shape))], axis=1)
    got = exchange(rows, FAR).astype(jnp.float32)

    sides = got[:, keep : keep + 4]
    total = jnp.sum(got[:, :keep] * jnp.exp2(sides[:, 2:3] - TOP), axis=0)
    losses = jnp.sum((sides[:, 0] + sides[:, 1] * (1.0 / LOW)) * jnp.exp2(sides[:, 3] - TOP), axis=0)
    return (total.reshape(-1, own_cols), steepness[:, :1] * error_proj, per_count[0] * losses)


def solution(mesh):
    finer = Mesh(mesh.devices.reshape(4, 4, 2, 6, 2, mesh.shape["mp"]), (*DP, "mp"))
    placed = (P(DP, "mp"), P("mp", None), P(DP, "mp"), P(DP, "mp"), P(DP, "mp"), P(DP))
    return jax.shard_map(
        body,
        mesh=finer,
        in_specs=placed,
        out_specs=(P(DP, "mp"), P(DP, "mp"), P()),
        check_vma=False,
    )
```

```python
import math

import jax
import jax.numpy as jnp
from jax import lax
from jax.experimental import pallas as pl
from jax.experimental.pallas import tpu as pltpu
from jax.sharding import Mesh
from jax.sharding import PartitionSpec as P

NBINS = 128
X, YH, YL, ZH, ZL = "dp_x", "dp_yh", "dp_yl", "dp_zh", "dp_zl"
DP = (X, YH, YL, ZH, ZL)
NEAR = (X, YL, ZL)
FAR = (YH, ZH)
LOSS_SCALE = 4096.0
ATTN_BOUND = 6.0
TOP = 14.0
SIDE = 8
LOW = 1024.0


def weights_at(index):
    centre = (index + 0.5) / NBINS
    logit = jnp.log(centre) - jnp.log(1.0 - centre)
    return jnp.exp(-0.5 * logit * logit) / (math.sqrt(2.0 * math.pi) * centre * (1.0 - centre))


def group(axes):
    return math.prod(lax.axis_size(a) for a in axes)


def partner(x):
    return lax.ppermute(x, "mp", [(0, 1), (1, 0)])


def exchange(x, axes):
    return lax.all_to_all(x, axes, 0, 0, tiled=True)


def exponent_of(bound):
    return jnp.floor(jnp.log2(jnp.maximum(bound, 1e-30))) + 2.0


def halves(scaled):
    high = lax.reduce_precision(scaled, 5, 10)
    return high, (scaled - high) * LOW


VMEM = pl.BlockSpec(memory_space=pltpu.VMEM)
SMEM = pl.BlockSpec(memory_space=pltpu.SMEM)
HBM = pl.BlockSpec(memory_space=pltpu.HBM)


def grant(mib):
    return pltpu.CompilerParams(vmem_limit_bytes=mib * 2**20)


def bin_lanes():
    return lax.broadcasted_iota(jnp.int32, (1, NBINS), 1)


def count_kernel(bins, spread):
    lane = bin_lanes()
    found = jnp.zeros((1, NBINS), jnp.float32)
    for s in range(bins.shape[0]):
        found = found + (lane == bins[s]).astype(jnp.float32)
    spread[...] = jnp.broadcast_to(found[None], spread.shape)


def fold_kernel(got, spread):
    spread[...] = jnp.broadcast_to(jnp.sum(got[...], axis=0, keepdims=True), spread.shape)


def count_sweep(bins):
    plane, column = (X, YH, YL), (ZH, ZL)
    spread = pl.pallas_call(
        count_kernel,
        out_shape=jax.ShapeDtypeStruct((group(plane), 1, NBINS), jnp.float32),
        in_specs=[SMEM],
        out_specs=VMEM,
        name="count",
    )(bins)
    got = exchange(spread, plane)
    spread = pl.pallas_call(
        fold_kernel,
        out_shape=jax.ShapeDtypeStruct((group(column), 1, NBINS), jnp.float32),
        in_specs=[VMEM],
        out_specs=VMEM,
        compiler_params=grant(2),
        name="fold",
    )(got)
    return exchange(spread, column)


def feature_rows(block, picks):
    run = picks.shape[0]
    for n in range(block.shape[1] // run):
        yield lax.dot_general(
            picks,
            block[:, n * run : (n + 1) * run],
            (((1,), (1,)), ((), ())),
            preferred_element_type=jnp.float32,
        ).astype(jnp.bfloat16)


def row_picks(run):
    row = lax.broadcasted_iota(jnp.int32, (run, run), 0)
    piece = (row * 683) >> 16
    inner = row - 96 * piece
    quad = inner >> 2
    y_high = (quad * 43) >> 8
    z_high = quad - 6 * y_high
    source = y_high * 96 + (piece >> 1) * 48 + z_high * 8 + (piece & 1) * 4 + (inner & 3)
    return (source == lax.broadcasted_iota(jnp.int32, (run, run), 1)).astype(jnp.bfloat16)


def forward_kernel(
    me,
    bins,
    attn_hbm,
    other_hbm,
    w_hbm,
    resid_hbm,
    target_hbm,
    gate,
    error,
    features_hbm,
    error_proj,
    marks,
    attn,
    attn_far,
    w_near,
    w_far,
    resid,
    target,
    features,
    load_sems,
    store_sems,
):
    tokens, half = attn.shape
    samples = gate.shape[0]
    per_sample = tokens // samples
    run = half // 2
    mine = pl.multiple_of(me[0] * half, half)
    theirs = pl.multiple_of((1 - me[0]) * half, half)
    pairs = (
        (attn_hbm, attn),
        (other_hbm.at[half:, :], attn_far),
        (w_hbm.at[:, pl.ds(mine, half)], w_near),
        (other_hbm.at[:half, :], w_far),
        (resid_hbm, resid),
        (target_hbm, target),
    )
    loads = [pltpu.make_async_copy(src, dst, load_sems.at[n]) for n, (src, dst) in enumerate(pairs)]
    for load in loads:
        load.start()
    stores = []

    def store(src, dst, rows):
        stores.append(pltpu.make_async_copy(src.at[rows, :], dst.at[rows, :], store_sems.at[len(stores)]))
        stores[-1].start()

    picks = row_picks(run)
    for first, block, load in ((mine, attn, loads[0]), (theirs, attn_far, loads[1])):
        load.wait()
        for n, moved in enumerate(feature_rows(block, picks)):
            features[pl.ds(pl.multiple_of(first + n * run, run), run), :] = moved
        store(features, features_hbm, pl.ds(first, half))
    for load in loads[2:]:
        load.wait()

    lane = bin_lanes()
    steepest = weights_at(lane.astype(jnp.float32)) * (LOSS_SCALE / (per_sample * half))
    found = jnp.zeros((1, NBINS), jnp.float32)
    reach = jnp.zeros((1, half), jnp.float32)
    for s in range(samples):
        rows = slice(s * per_sample, (s + 1) * per_sample)
        projected = jnp.dot(attn[rows, :], w_near[...], preferred_element_type=jnp.float32) + jnp.dot(
            attn_far[rows, :], w_far[...], preferred_element_type=jnp.float32
        )
        scale = gate[s : s + 1, :]
        diff = resid[rows, :].astype(jnp.float32) + scale * projected - target[rows, :].astype(jnp.float32)
        error[rows, :] = diff
        error_proj[s : s + 1, :] = jnp.sum(diff * projected, axis=0, keepdims=True)
        hit = lane == bins[s]
        largest = jnp.sum(jnp.where(hit, steepest, 0.0), axis=1, keepdims=True)
        reach = reach + largest * jnp.sum(jnp.abs(diff * scale), axis=0, keepdims=True)
        squares = jnp.sum(jnp.sum(diff * diff, axis=0, keepdims=True), axis=1, keepdims=True)
        found = found + jnp.where(hit, squares * (1.0 / (per_sample * 2 * half)), 0.0)
    bound = exponent_of(jnp.max(reach, axis=1, keepdims=True) * (1.01 * ATTN_BOUND))
    marks[...] = jnp.broadcast_to(bound, marks.shape)
    marks[:1, :] = found
    for copy in stores:
        copy.wait()


def forward(me, bins, attn, other, w_out, resid, target, gate):
    tokens, half = attn.shape
    block = pltpu.VMEM(attn.shape, attn.dtype)
    square = pltpu.VMEM((half, half), attn.dtype)
    return pl.pallas_call(
        forward_kernel,
        out_shape=(
            jax.ShapeDtypeStruct((tokens, half), jnp.float32),
            jax.ShapeDtypeStruct((2 * half, tokens), jnp.bfloat16),
            jax.ShapeDtypeStruct(gate.shape, jnp.float32),
            jax.ShapeDtypeStruct((SIDE, NBINS), jnp.float32),
        ),
        in_specs=[SMEM] * 2 + [HBM] * 5 + [VMEM],
        out_specs=(VMEM, HBM, VMEM, VMEM),
        scratch_shapes=[
            block,
            block,
            square,
            square,
            block,
            block,
            pltpu.VMEM((2 * half, tokens), jnp.bfloat16),
            pltpu.SemaphoreType.DMA((6,)),
            pltpu.SemaphoreType.DMA((2,)),
        ],
        cost_estimate=pl.CostEstimate(flops=10**9, bytes_accessed=6 * 10**6, transcendentals=0),
        compiler_params=grant(50),
        name="forward",
    )(me, bins, attn, other, w_out, resid, target, gate)


def scale_kernel(
    bins, got, marks, other_marks, error, gate, d_proj, steepness, per_count, side
):
    tokens, half = error.shape
    samples = gate.shape[0]
    per_sample = tokens // samples
    lane = bin_lanes()
    floored = jnp.maximum(jnp.sum(got[...], axis=0), 1.0)
    slope = weights_at(lane.astype(jnp.float32)) / floored
    per_count[...] = slope
    grad_exp = marks[1:2, :]
    lift = jnp.exp2(TOP - grad_exp[:, :1])
    for s in range(samples):
        rows = slice(s * per_sample, (s + 1) * per_sample)
        coefficient = jnp.sum(jnp.where(lane == bins[s], slope * LOSS_SCALE, 0.0), axis=1, keepdims=True)
        coefficient = coefficient * (1.0 / (per_sample * half))
        rounded = (coefficient * error[rows, :] * gate[s : s + 1, :]).astype(jnp.bfloat16)
        d_proj[rows, :] = (rounded.astype(jnp.float32) * lift).astype(jnp.bfloat16)
        steepness[s : s + 1, :] = jnp.broadcast_to(coefficient, (1, NBINS))
    total = marks[:1, :] + other_marks[:1, :]
    loss_exp = exponent_of(total)
    high, low = halves(total * jnp.exp2(TOP - loss_exp))
    side[...] = jnp.zeros(side.shape, jnp.float32)
    for n, row in enumerate((high, low, grad_exp, loss_exp)):
        side[n : n + 1, :] = row


def scaled(bins, got, marks, other_marks, error, gate):
    return pl.pallas_call(
        scale_kernel,
        out_shape=(
            jax.ShapeDtypeStruct(error.shape, jnp.bfloat16),
            jax.ShapeDtypeStruct((gate.shape[0], NBINS), jnp.float32),
            jax.ShapeDtypeStruct((1, NBINS), jnp.float32),
            jax.ShapeDtypeStruct((SIDE, NBINS), jnp.float32),
        ),
        in_specs=[SMEM] + [VMEM] * 5,
        out_specs=(VMEM,) * 4,
        cost_estimate=pl.CostEstimate(flops=10**7, bytes_accessed=2 * 10**6, transcendentals=0),
        compiler_params=grant(20),
        name="scaled",
    )(bins, got, marks, other_marks, error, gate)


def body(attn, w_out, resid, target, gate, bins):
    own_cols = resid.shape[1]
    me = lax.axis_index("mp")
    got = count_sweep(bins)
    w_theirs = lax.dynamic_slice_in_dim(w_out, (1 - me) * own_cols, own_cols, axis=1)
    other = partner(jnp.concatenate([w_theirs, attn], axis=0))
    error, features, error_proj, marks = forward(
        me.reshape(1), bins, attn, other, w_out, resid, target, gate
    )
    other_marks = partner(marks)
    near, far = group(NEAR), group(FAR)
    d_proj, steepness, per_count, side = scaled(bins, got, marks, other_marks, error, gate)
    side = side.astype(jnp.float16)
    partial = jnp.dot(features, d_proj, preferred_element_type=jnp.float32)
    partial = partial.astype(jnp.float16).reshape(near, -1, SIDE, own_cols)
    stripes = partial.shape[1]
    partial = partial.transpose(0, 2, 1, 3).reshape(near, SIDE, stripes * own_cols)
    partial = jnp.concatenate([partial, jnp.broadcast_to(side[None], (near, *side.shape))], axis=2)
    got = exchange(partial, NEAR)

    sides = got[:, :4, stripes * own_cols :].astype(jnp.float32)
    grad_exp = jnp.max(sides[:, 2], axis=0) + math.log2(near)
    scale = jnp.exp2(sides[:, 2, :1] - grad_exp[:1])
    got = got[:, :, : stripes * own_cols].astype(jnp.float32)
    total = jnp.sum(got * scale[:, :, None], axis=0)
    loss_exp = jnp.max(sides[:, 3], axis=0) + math.log2(near)
    high, low = halves(
        jnp.sum((sides[:, 0] + sides[:, 1] * (1.0 / LOW)) * jnp.exp2(sides[:, 3] - loss_exp), axis=0)
    )
    side = jnp.stack([high, low, grad_exp, loss_exp])
    side = jnp.pad(side, ((0, SIDE - 4), (0, 0))).astype(jnp.float16)
    rows = total.astype(jnp.float16).reshape(SIDE, stripes, own_cols).transpose(1, 0, 2)
    rows = rows.reshape(far, -1, NBINS)
    keep = rows.shape[1]
    rows = jnp.concatenate([rows, jnp.broadcast_to(side[None], (far, *side.shape))], axis=1)
    got = exchange(rows, FAR).astype(jnp.float32)

    sides = got[:, keep : keep + 4]
    total = jnp.sum(got[:, :keep] * jnp.exp2(sides[:, 2:3] - TOP), axis=0)
    losses = jnp.sum((sides[:, 0] + sides[:, 1] * (1.0 / LOW)) * jnp.exp2(sides[:, 3] - TOP), axis=0)
    return (total.reshape(-1, own_cols), steepness[:, :1] * error_proj, per_count[0] * losses)


def solution(mesh):
    finer = Mesh(mesh.devices.reshape(4, 4, 2, 6, 2, mesh.shape["mp"]), (*DP, "mp"))
    placed = (P(DP, "mp"), P("mp", None), P(DP, "mp"), P(DP, "mp"), P(DP, "mp"), P(DP))
    return jax.shard_map(
        body,
        mesh=finer,
        in_specs=placed,
        out_specs=(P(DP, "mp"), P(DP, "mp"), P()),
        check_vma=False,
    )
```

```python
import math

import jax
import jax.numpy as jnp
from jax import lax
from jax.experimental import pallas as pl
from jax.experimental.pallas import tpu as pltpu
from jax.sharding import Mesh
from jax.sharding import PartitionSpec as P

NBINS = 128
X, YH, YL, ZH, ZL = "dp_x", "dp_yh", "dp_yl", "dp_zh", "dp_zl"
DP = (X, YH, YL, ZH, ZL)
NEAR = (X, YL, ZL)
FAR = (YH, ZH)
LOSS_SCALE = 4096.0
ATTN_BOUND = 6.0
TOP = 14.0
SIDE = 8
LOW = 1024.0


def weights_at(index):
    centre = (index + 0.5) / NBINS
    logit = jnp.log(centre) - jnp.log(1.0 - centre)
    return jnp.exp(-0.5 * logit * logit) / (math.sqrt(2.0 * math.pi) * centre * (1.0 - centre))


def group(axes):
    return math.prod(lax.axis_size(a) for a in axes)


def partner(x):
    return lax.ppermute(x, "mp", [(0, 1), (1, 0)])


def exchange(x, axes):
    return lax.all_to_all(x, axes, 0, 0, tiled=True)


def exponent_of(bound):
    return jnp.floor(jnp.log2(jnp.maximum(bound, 1e-30))) + 2.0


def halves(scaled):
    high = lax.reduce_precision(scaled, 5, 10)
    return high, (scaled - high) * LOW


VMEM = pl.BlockSpec(memory_space=pltpu.VMEM)
SMEM = pl.BlockSpec(memory_space=pltpu.SMEM)
HBM = pl.BlockSpec(memory_space=pltpu.HBM)


def grant(mib):
    return pltpu.CompilerParams(vmem_limit_bytes=mib * 2**20)


def bin_lanes():
    return lax.broadcasted_iota(jnp.int32, (1, NBINS), 1)


def count_kernel(bins, spread):
    lane = bin_lanes()
    found = jnp.zeros((1, NBINS), jnp.float32)
    for s in range(bins.shape[0]):
        found = found + (lane == bins[s]).astype(jnp.float32)
    spread[...] = jnp.broadcast_to(found[None], spread.shape)


def fold_kernel(got, spread):
    spread[...] = jnp.broadcast_to(jnp.sum(got[...], axis=0, keepdims=True), spread.shape)


def count_sweep(bins):
    plane, column = (X, YH, YL), (ZH, ZL)
    spread = pl.pallas_call(
        count_kernel,
        out_shape=jax.ShapeDtypeStruct((group(plane), 1, NBINS), jnp.float32),
        in_specs=[SMEM],
        out_specs=VMEM,
        name="count",
    )(bins)
    got = exchange(spread, plane)
    spread = pl.pallas_call(
        fold_kernel,
        out_shape=jax.ShapeDtypeStruct((group(column), 1, NBINS), jnp.float32),
        in_specs=[VMEM],
        out_specs=VMEM,
        compiler_params=grant(2),
        name="fold",
    )(got)
    return exchange(spread, column)


def feature_rows(block, picks):
    run = picks.shape[0]
    for n in range(block.shape[1] // run):
        yield lax.dot_general(
            picks,
            block[:, n * run : (n + 1) * run],
            (((1,), (1,)), ((), ())),
            preferred_element_type=jnp.float32,
        ).astype(jnp.bfloat16)


def row_picks(run):
    row = lax.broadcasted_iota(jnp.int32, (run, run), 0)
    piece = (row * 683) >> 16
    inner = row - 96 * piece
    quad = inner >> 2
    y_high = (quad * 43) >> 8
    z_high = quad - 6 * y_high
    source = y_high * 96 + (piece >> 1) * 48 + z_high * 8 + (piece & 1) * 4 + (inner & 3)
    return (source == lax.broadcasted_iota(jnp.int32, (run, run), 1)).astype(jnp.bfloat16)


def pack_kernel(me, w_hbm, attn_hbm, send):
    half = attn_hbm.shape[1]
    theirs = pl.multiple_of((1 - me[0]) * half, half)
    parts = 4

    def body(sems):
        copies = []
        for src, top in ((w_hbm.at[:, pl.ds(theirs, half)], 0), (attn_hbm, half)):
            step = src.shape[0] // parts
            for n in range(parts):
                rows = pl.ds(n * step, step)
                copies.append(
                    pltpu.make_async_copy(
                        src.at[rows, :], send.at[pl.ds(top + n * step, step), :], sems.at[len(copies)]
                    )
                )
                copies[-1].start()
        for copy in copies:
            copy.wait()

    pl.run_scoped(body, pltpu.SemaphoreType.DMA((2 * parts,)))


def packed(me, w_out, attn):
    tokens, half = attn.shape
    return pl.pallas_call(
        pack_kernel,
        out_shape=jax.ShapeDtypeStruct((half + tokens, half), attn.dtype),
        in_specs=[SMEM, HBM, HBM],
        out_specs=HBM,
        cost_estimate=pl.CostEstimate(flops=10**7, bytes_accessed=4 * 10**6, transcendentals=0),
        name="packed",
    )(me, w_out, attn)


def forward_kernel(
    me,
    bins,
    attn_hbm,
    other_hbm,
    w_hbm,
    resid_hbm,
    target_hbm,
    gate,
    error,
    features_hbm,
    error_proj,
    marks,
    attn,
    attn_far,
    w_near,
    w_far,
    resid,
    target,
    features,
    load_sems,
    store_sems,
):
    tokens, half = attn.shape
    samples = gate.shape[0]
    per_sample = tokens // samples
    run = half // 2
    mine = pl.multiple_of(me[0] * half, half)
    theirs = pl.multiple_of((1 - me[0]) * half, half)
    pairs = (
        (attn_hbm, attn),
        (other_hbm.at[half:, :], attn_far),
        (w_hbm.at[:, pl.ds(mine, half)], w_near),
        (other_hbm.at[:half, :], w_far),
        (resid_hbm, resid),
        (target_hbm, target),
    )
    loads = [pltpu.make_async_copy(src, dst, load_sems.at[n]) for n, (src, dst) in enumerate(pairs)]
    for load in loads:
        load.start()
    stores = []

    def store(src, dst, rows):
        stores.append(pltpu.make_async_copy(src.at[rows, :], dst.at[rows, :], store_sems.at[len(stores)]))
        stores[-1].start()

    picks = row_picks(run)
    for first, block, load in ((mine, attn, loads[0]), (theirs, attn_far, loads[1])):
        load.wait()
        for n, moved in enumerate(feature_rows(block, picks)):
            features[pl.ds(pl.multiple_of(first + n * run, run), run), :] = moved
        store(features, features_hbm, pl.ds(first, half))
    for load in loads[2:]:
        load.wait()

    lane = bin_lanes()
    steepest = weights_at(lane.astype(jnp.float32)) * (LOSS_SCALE / (per_sample * half))
    found = jnp.zeros((1, NBINS), jnp.float32)
    reach = jnp.zeros((1, half), jnp.float32)
    for s in range(samples):
        rows = slice(s * per_sample, (s + 1) * per_sample)
        projected = jnp.dot(attn[rows, :], w_near[...], preferred_element_type=jnp.float32) + jnp.dot(
            attn_far[rows, :], w_far[...], preferred_element_type=jnp.float32
        )
        scale = gate[s : s + 1, :]
        diff = resid[rows, :].astype(jnp.float32) + scale * projected - target[rows, :].astype(jnp.float32)
        error[rows, :] = diff
        error_proj[s : s + 1, :] = jnp.sum(diff * projected, axis=0, keepdims=True)
        hit = lane == bins[s]
        largest = jnp.sum(jnp.where(hit, steepest, 0.0), axis=1, keepdims=True)
        reach = reach + largest * jnp.sum(jnp.abs(diff * scale), axis=0, keepdims=True)
        squares = jnp.sum(jnp.sum(diff * diff, axis=0, keepdims=True), axis=1, keepdims=True)
        found = found + jnp.where(hit, squares * (1.0 / (per_sample * 2 * half)), 0.0)
    bound = exponent_of(jnp.max(reach, axis=1, keepdims=True) * (1.01 * ATTN_BOUND))
    marks[...] = jnp.broadcast_to(bound, marks.shape)
    marks[:1, :] = found
    for copy in stores:
        copy.wait()


def forward(me, bins, attn, other, w_out, resid, target, gate):
    tokens, half = attn.shape
    block = pltpu.VMEM(attn.shape, attn.dtype)
    square = pltpu.VMEM((half, half), attn.dtype)
    return pl.pallas_call(
        forward_kernel,
        out_shape=(
            jax.ShapeDtypeStruct((tokens, half), jnp.float32),
            jax.ShapeDtypeStruct((2 * half, tokens), jnp.bfloat16),
            jax.ShapeDtypeStruct(gate.shape, jnp.float32),
            jax.ShapeDtypeStruct((SIDE, NBINS), jnp.float32),
        ),
        in_specs=[SMEM] * 2 + [HBM] * 5 + [VMEM],
        out_specs=(VMEM, HBM, VMEM, VMEM),
        scratch_shapes=[
            block,
            block,
            square,
            square,
            block,
            block,
            pltpu.VMEM((2 * half, tokens), jnp.bfloat16),
            pltpu.SemaphoreType.DMA((6,)),
            pltpu.SemaphoreType.DMA((2,)),
        ],
        cost_estimate=pl.CostEstimate(flops=10**9, bytes_accessed=6 * 10**6, transcendentals=0),
        compiler_params=grant(50),
        name="forward",
    )(me, bins, attn, other, w_out, resid, target, gate)


def scale_kernel(
    bins, got, marks, other_marks, error, gate, d_proj, steepness, per_count, side
):
    tokens, half = error.shape
    samples = gate.shape[0]
    per_sample = tokens // samples
    lane = bin_lanes()
    floored = jnp.maximum(jnp.sum(got[...], axis=0), 1.0)
    slope = weights_at(lane.astype(jnp.float32)) / floored
    per_count[...] = slope
    grad_exp = marks[1:2, :]
    lift = jnp.exp2(TOP - grad_exp[:, :1])
    for s in range(samples):
        rows = slice(s * per_sample, (s + 1) * per_sample)
        coefficient = jnp.sum(jnp.where(lane == bins[s], slope * LOSS_SCALE, 0.0), axis=1, keepdims=True)
        coefficient = coefficient * (1.0 / (per_sample * half))
        rounded = (coefficient * error[rows, :] * gate[s : s + 1, :]).astype(jnp.bfloat16)
        d_proj[rows, :] = (rounded.astype(jnp.float32) * lift).astype(jnp.bfloat16)
        steepness[s : s + 1, :] = jnp.broadcast_to(coefficient, (1, NBINS))
    total = marks[:1, :] + other_marks[:1, :]
    loss_exp = exponent_of(total)
    high, low = halves(total * jnp.exp2(TOP - loss_exp))
    side[...] = jnp.zeros(side.shape, jnp.float32)
    for n, row in enumerate((high, low, grad_exp, loss_exp)):
        side[n : n + 1, :] = row


def scaled(bins, got, marks, other_marks, error, gate):
    return pl.pallas_call(
        scale_kernel,
        out_shape=(
            jax.ShapeDtypeStruct(error.shape, jnp.bfloat16),
            jax.ShapeDtypeStruct((gate.shape[0], NBINS), jnp.float32),
            jax.ShapeDtypeStruct((1, NBINS), jnp.float32),
            jax.ShapeDtypeStruct((SIDE, NBINS), jnp.float32),
        ),
        in_specs=[SMEM] + [VMEM] * 5,
        out_specs=(VMEM,) * 4,
        cost_estimate=pl.CostEstimate(flops=10**7, bytes_accessed=2 * 10**6, transcendentals=0),
        compiler_params=grant(20),
        name="scaled",
    )(bins, got, marks, other_marks, error, gate)


def body(attn, w_out, resid, target, gate, bins):
    own_cols = resid.shape[1]
    me = lax.axis_index("mp")
    got = count_sweep(bins)
    other = partner(packed(me.reshape(1), w_out, attn))
    error, features, error_proj, marks = forward(
        me.reshape(1), bins, attn, other, w_out, resid, target, gate
    )
    other_marks = partner(marks)
    near, far = group(NEAR), group(FAR)
    d_proj, steepness, per_count, side = scaled(bins, got, marks, other_marks, error, gate)
    side = side.astype(jnp.float16)
    partial = jnp.dot(features, d_proj, preferred_element_type=jnp.float32)
    partial = partial.astype(jnp.float16).reshape(near, -1, SIDE, own_cols)
    stripes = partial.shape[1]
    partial = partial.transpose(0, 2, 1, 3).reshape(near, SIDE, stripes * own_cols)
    partial = jnp.concatenate([partial, jnp.broadcast_to(side[None], (near, *side.shape))], axis=2)
    got = exchange(partial, NEAR)

    sides = got[:, :4, stripes * own_cols :].astype(jnp.float32)
    grad_exp = jnp.max(sides[:, 2], axis=0) + math.log2(near)
    scale = jnp.exp2(sides[:, 2, :1] - grad_exp[:1])
    got = got[:, :, : stripes * own_cols].astype(jnp.float32)
    total = jnp.sum(got * scale[:, :, None], axis=0)
    loss_exp = jnp.max(sides[:, 3], axis=0) + math.log2(near)
    high, low = halves(
        jnp.sum((sides[:, 0] + sides[:, 1] * (1.0 / LOW)) * jnp.exp2(sides[:, 3] - loss_exp), axis=0)
    )
    side = jnp.stack([high, low, grad_exp, loss_exp]).astype(jnp.float16)
    rows = total.astype(jnp.float16).reshape(SIDE, stripes, own_cols).transpose(1, 0, 2)
    rows = rows.reshape(far, -1, own_cols)
    rows = jnp.concatenate([rows, jnp.broadcast_to(side[None], (far, *side.shape))], axis=2)
    got = exchange(rows, FAR).astype(jnp.float32)

    sides = got[:, :, own_cols:]
    total = jnp.sum(got[:, :, :own_cols] * jnp.exp2(sides[:, 2:3, :1] - TOP), axis=0)
    losses = jnp.sum((sides[:, 0] + sides[:, 1] * (1.0 / LOW)) * jnp.exp2(sides[:, 3] - TOP), axis=0)
    return (total, steepness[:, :1] * error_proj, per_count[0] * losses)


def solution(mesh):
    finer = Mesh(mesh.devices.reshape(4, 4, 2, 6, 2, mesh.shape["mp"]), (*DP, "mp"))
    placed = (P(DP, "mp"), P("mp", None), P(DP, "mp"), P(DP, "mp"), P(DP, "mp"), P(DP))
    return jax.shard_map(
        body,
        mesh=finer,
        in_specs=placed,
        out_specs=(P(DP, "mp"), P(DP, "mp"), P()),
        check_vma=False,
    )
```

```python
import math

import jax
import jax.numpy as jnp
from jax import lax
from jax.experimental import pallas as pl
from jax.experimental.pallas import tpu as pltpu
from jax.sharding import Mesh
from jax.sharding import PartitionSpec as P

NBINS = 128
X, YH, YL, ZH, ZL = "dp_x", "dp_yh", "dp_yl", "dp_zh", "dp_zl"
DP = (X, YH, YL, ZH, ZL)
NEAR = (X, YL, ZL)
FAR = (YH, ZH)
LOSS_SCALE = 4096.0
ATTN_BOUND = 6.0
TOP = 14.0
SIDE = 8
LOW = 1024.0


def weights_at(index):
    centre = (index + 0.5) / NBINS
    logit = jnp.log(centre) - jnp.log(1.0 - centre)
    return jnp.exp(-0.5 * logit * logit) / (math.sqrt(2.0 * math.pi) * centre * (1.0 - centre))


def group(axes):
    return math.prod(lax.axis_size(a) for a in axes)


def partner(x):
    return lax.ppermute(x, "mp", [(0, 1), (1, 0)])


def exchange(x, axes):
    return lax.all_to_all(x, axes, 0, 0, tiled=True)


def exponent_of(bound):
    return jnp.floor(jnp.log2(jnp.maximum(bound, 1e-30))) + 2.0


def halves(scaled):
    high = lax.reduce_precision(scaled, 5, 10)
    return high, (scaled - high) * LOW


VMEM = pl.BlockSpec(memory_space=pltpu.VMEM)
SMEM = pl.BlockSpec(memory_space=pltpu.SMEM)
HBM = pl.BlockSpec(memory_space=pltpu.HBM)


def grant(mib):
    return pltpu.CompilerParams(vmem_limit_bytes=mib * 2**20)


def bin_lanes():
    return lax.broadcasted_iota(jnp.int32, (1, NBINS), 1)


def count_kernel(bins, spread):
    lane = bin_lanes()
    found = jnp.zeros((1, NBINS), jnp.float32)
    for s in range(bins.shape[0]):
        found = found + (lane == bins[s]).astype(jnp.float32)
    spread[...] = jnp.broadcast_to(found[None], spread.shape)


def fold_kernel(got, spread):
    spread[...] = jnp.broadcast_to(jnp.sum(got[...], axis=0, keepdims=True), spread.shape)


def count_sweep(bins):
    plane, column = (ZH, ZL), (X, YH, YL)
    spread = pl.pallas_call(
        count_kernel,
        out_shape=jax.ShapeDtypeStruct((group(plane), 1, NBINS), jnp.float32),
        in_specs=[SMEM],
        out_specs=VMEM,
        name="count",
    )(bins)
    got = exchange(spread, plane)
    spread = pl.pallas_call(
        fold_kernel,
        out_shape=jax.ShapeDtypeStruct((group(column), 1, NBINS), jnp.float32),
        in_specs=[VMEM],
        out_specs=VMEM,
        compiler_params=grant(2),
        name="fold",
    )(got)
    return exchange(spread, column)


def feature_rows(block, picks):
    run = picks.shape[0]
    for n in range(block.shape[1] // run):
        yield lax.dot_general(
            picks,
            block[:, n * run : (n + 1) * run],
            (((1,), (1,)), ((), ())),
            preferred_element_type=jnp.float32,
        ).astype(jnp.bfloat16)


def row_picks(run):
    row = lax.broadcasted_iota(jnp.int32, (run, run), 0)
    piece = (row * 683) >> 16
    inner = row - 96 * piece
    quad = inner >> 2
    y_high = (quad * 43) >> 8
    z_high = quad - 6 * y_high
    source = y_high * 96 + (piece >> 1) * 48 + z_high * 8 + (piece & 1) * 4 + (inner & 3)
    return (source == lax.broadcasted_iota(jnp.int32, (run, run), 1)).astype(jnp.bfloat16)


def forward_kernel(
    me,
    bins,
    attn_hbm,
    other_hbm,
    w_hbm,
    resid_hbm,
    target_hbm,
    gate,
    error,
    features_hbm,
    error_proj,
    marks,
    attn,
    attn_far,
    w_near,
    w_far,
    resid,
    target,
    features,
    load_sems,
    store_sems,
):
    tokens, half = attn.shape
    samples = gate.shape[0]
    per_sample = tokens // samples
    run = half // 2
    mine = pl.multiple_of(me[0] * half, half)
    theirs = pl.multiple_of((1 - me[0]) * half, half)
    pairs = (
        (attn_hbm, attn),
        (other_hbm.at[half:, :], attn_far),
        (w_hbm.at[:, pl.ds(mine, half)], w_near),
        (other_hbm.at[:half, :], w_far),
        (resid_hbm, resid),
        (target_hbm, target),
    )
    loads = [pltpu.make_async_copy(src, dst, load_sems.at[n]) for n, (src, dst) in enumerate(pairs)]
    for load in loads:
        load.start()
    stores = []

    def store(src, dst, rows):
        stores.append(pltpu.make_async_copy(src.at[rows, :], dst.at[rows, :], store_sems.at[len(stores)]))
        stores[-1].start()

    picks = row_picks(run)
    for first, block, load in ((mine, attn, loads[0]), (theirs, attn_far, loads[1])):
        load.wait()
        for n, moved in enumerate(feature_rows(block, picks)):
            features[pl.ds(pl.multiple_of(first + n * run, run), run), :] = moved
        store(features, features_hbm, pl.ds(first, half))
    for load in loads[2:]:
        load.wait()

    lane = bin_lanes()
    steepest = weights_at(lane.astype(jnp.float32)) * (LOSS_SCALE / (per_sample * half))
    found = jnp.zeros((1, NBINS), jnp.float32)
    reach = jnp.zeros((1, half), jnp.float32)
    for s in range(samples):
        rows = slice(s * per_sample, (s + 1) * per_sample)
        projected = jnp.dot(attn[rows, :], w_near[...], preferred_element_type=jnp.float32) + jnp.dot(
            attn_far[rows, :], w_far[...], preferred_element_type=jnp.float32
        )
        scale = gate[s : s + 1, :]
        diff = resid[rows, :].astype(jnp.float32) + scale * projected - target[rows, :].astype(jnp.float32)
        error[rows, :] = diff
        error_proj[s : s + 1, :] = jnp.sum(diff * projected, axis=0, keepdims=True)
        hit = lane == bins[s]
        largest = jnp.sum(jnp.where(hit, steepest, 0.0), axis=1, keepdims=True)
        reach = reach + largest * jnp.sum(jnp.abs(diff * scale), axis=0, keepdims=True)
        squares = jnp.sum(jnp.sum(diff * diff, axis=0, keepdims=True), axis=1, keepdims=True)
        found = found + jnp.where(hit, squares * (1.0 / (per_sample * 2 * half)), 0.0)
    bound = exponent_of(jnp.max(reach, axis=1, keepdims=True) * (1.01 * ATTN_BOUND))
    marks[...] = jnp.broadcast_to(bound, marks.shape)
    marks[:1, :] = found
    for copy in stores:
        copy.wait()


def forward(me, bins, attn, other, w_out, resid, target, gate):
    tokens, half = attn.shape
    block = pltpu.VMEM(attn.shape, attn.dtype)
    square = pltpu.VMEM((half, half), attn.dtype)
    return pl.pallas_call(
        forward_kernel,
        out_shape=(
            jax.ShapeDtypeStruct((tokens, half), jnp.float32),
            jax.ShapeDtypeStruct((2 * half, tokens), jnp.bfloat16),
            jax.ShapeDtypeStruct(gate.shape, jnp.float32),
            jax.ShapeDtypeStruct((SIDE, NBINS), jnp.float32),
        ),
        in_specs=[SMEM] * 2 + [HBM] * 5 + [VMEM],
        out_specs=(VMEM, HBM, VMEM, VMEM),
        scratch_shapes=[
            block,
            block,
            square,
            square,
            block,
            block,
            pltpu.VMEM((2 * half, tokens), jnp.bfloat16),
            pltpu.SemaphoreType.DMA((6,)),
            pltpu.SemaphoreType.DMA((2,)),
        ],
        cost_estimate=pl.CostEstimate(flops=10**9, bytes_accessed=6 * 10**6, transcendentals=0),
        compiler_params=grant(50),
        name="forward",
    )(me, bins, attn, other, w_out, resid, target, gate)


def scale_kernel(
    bins, got, marks, other_marks, error, gate, d_proj, steepness, per_count, side
):
    tokens, half = error.shape
    samples = gate.shape[0]
    per_sample = tokens // samples
    lane = bin_lanes()
    floored = jnp.maximum(jnp.sum(got[...], axis=0), 1.0)
    slope = weights_at(lane.astype(jnp.float32)) / floored
    per_count[...] = slope
    grad_exp = marks[1:2, :]
    lift = jnp.exp2(TOP - grad_exp[:, :1])
    for s in range(samples):
        rows = slice(s * per_sample, (s + 1) * per_sample)
        coefficient = jnp.sum(jnp.where(lane == bins[s], slope * LOSS_SCALE, 0.0), axis=1, keepdims=True)
        coefficient = coefficient * (1.0 / (per_sample * half))
        rounded = (coefficient * error[rows, :] * gate[s : s + 1, :]).astype(jnp.bfloat16)
        d_proj[rows, :] = (rounded.astype(jnp.float32) * lift).astype(jnp.bfloat16)
        steepness[s : s + 1, :] = jnp.broadcast_to(coefficient, (1, NBINS))
    total = marks[:1, :] + other_marks[:1, :]
    loss_exp = exponent_of(total)
    high, low = halves(total * jnp.exp2(TOP - loss_exp))
    side[...] = jnp.zeros(side.shape, jnp.float32)
    for n, row in enumerate((high, low, grad_exp, loss_exp)):
        side[n : n + 1, :] = row


def scaled(bins, got, marks, other_marks, error, gate):
    return pl.pallas_call(
        scale_kernel,
        out_shape=(
            jax.ShapeDtypeStruct(error.shape, jnp.bfloat16),
            jax.ShapeDtypeStruct((gate.shape[0], NBINS), jnp.float32),
            jax.ShapeDtypeStruct((1, NBINS), jnp.float32),
            jax.ShapeDtypeStruct((SIDE, NBINS), jnp.float32),
        ),
        in_specs=[SMEM] + [VMEM] * 5,
        out_specs=(VMEM,) * 4,
        cost_estimate=pl.CostEstimate(flops=10**7, bytes_accessed=2 * 10**6, transcendentals=0),
        compiler_params=grant(20),
        name="scaled",
    )(bins, got, marks, other_marks, error, gate)


def body(attn, w_out, resid, target, gate, bins):
    own_cols = resid.shape[1]
    me = lax.axis_index("mp")
    got = count_sweep(bins)
    w_theirs = lax.dynamic_slice_in_dim(w_out, (1 - me) * own_cols, own_cols, axis=1)
    other = partner(jnp.concatenate([w_theirs, attn], axis=0))
    error, features, error_proj, marks = forward(
        me.reshape(1), bins, attn, other, w_out, resid, target, gate
    )
    other_marks = partner(marks)
    near, far = group(NEAR), group(FAR)
    d_proj, steepness, per_count, side = scaled(bins, got, marks, other_marks, error, gate)
    side = side.astype(jnp.float16)
    partial = jnp.dot(features, d_proj, preferred_element_type=jnp.float32)
    partial = partial.astype(jnp.float16).reshape(near, -1, SIDE, own_cols)
    stripes = partial.shape[1]
    partial = partial.transpose(0, 2, 1, 3).reshape(near, SIDE, stripes * own_cols)
    partial = jnp.concatenate([partial, jnp.broadcast_to(side[None], (near, *side.shape))], axis=2)
    got = exchange(partial, NEAR)

    sides = got[:, :4, stripes * own_cols :].astype(jnp.float32)
    grad_exp = jnp.max(sides[:, 2], axis=0) + math.log2(near)
    scale = jnp.exp2(sides[:, 2, :1] - grad_exp[:1])
    got = got[:, :, : stripes * own_cols].astype(jnp.float32)
    total = jnp.sum(got * scale[:, :, None], axis=0)
    loss_exp = jnp.max(sides[:, 3], axis=0) + math.log2(near)
    high, low = halves(
        jnp.sum((sides[:, 0] + sides[:, 1] * (1.0 / LOW)) * jnp.exp2(sides[:, 3] - loss_exp), axis=0)
    )
    side = jnp.stack([high, low, grad_exp, loss_exp]).astype(jnp.float16)
    rows = total.astype(jnp.float16).reshape(SIDE, stripes, own_cols).transpose(1, 0, 2)
    rows = rows.reshape(far, -1, own_cols)
    rows = jnp.concatenate([rows, jnp.broadcast_to(side[None], (far, *side.shape))], axis=2)
    got = exchange(rows, FAR).astype(jnp.float32)

    sides = got[:, :, own_cols:]
    total = jnp.sum(got[:, :, :own_cols] * jnp.exp2(sides[:, 2:3, :1] - TOP), axis=0)
    losses = jnp.sum((sides[:, 0] + sides[:, 1] * (1.0 / LOW)) * jnp.exp2(sides[:, 3] - TOP), axis=0)
    return (total, steepness[:, :1] * error_proj, per_count[0] * losses)


def solution(mesh):
    finer = Mesh(mesh.devices.reshape(4, 4, 2, 6, 2, mesh.shape["mp"]), (*DP, "mp"))
    placed = (P(DP, "mp"), P("mp", None), P(DP, "mp"), P(DP, "mp"), P(DP, "mp"), P(DP))
    return jax.shard_map(
        body,
        mesh=finer,
        in_specs=placed,
        out_specs=(P(DP, "mp"), P(DP, "mp"), P()),
        check_vma=False,
    )
```
